512 devices in a mesh: dp: 16 (over y, core), space: 32 (over z, x).
Axes of the slice: x: 4, y: 8, z: 8, core: 2. Of those that a mesh axis runs over, the one named last changes fastest.
Arguments:
- features: bfloat16 [16, 32, 48, 512], P('dp', 'space'), may hold values from -6 to 6
- device_block: int32 [16, 32], P('dp'), may hold values from 0 to 63, as said below
- conv_first: bfloat16 [48, 27, 48], replicated, may hold values from -0.15625 to 0.15625
- conv_second: bfloat16 [48, 27, 48], replicated, may hold values from -0.15625 to 0.15625
- head_weight: bfloat16 [3, 48], replicated, may hold values from -0.875 to 0.875
- targets: int32 [16, 32, 3, 512], P('dp', 'space'), may hold values 0 or 1
Outputs:
- affinity_logits: float32 [16, 32, 3, 512], P('dp', 'space')
- grad_first: float32 [48, 27, 48], replicated
- grad_second: float32 [48, 27, 48], replicated
- grad_head: float32 [3, 48], replicated
The draws below stay inside these ranges and needn't reach their ends.
Inputs may be any that keep to these rules, and one draw needn't show every extreme that they name: `device_block`: row n lists 32 distinct block ids of crop n, one for each device; id = (4 * bx + by) * 4 + bz. Blocks that no device lists hold no tissue.
All inputs are finite; a program needn't handle non-finite values. No bound on the sum of `targets` on one device may be relied on, other than what follows from the above.
Results may differ from the reference program's by a relative error of at most 0.0041.
Values may be sent and summed in bfloat16 or wider, within the bound.
A program may use at most 64 MiB of HBM per device.

```python
import jax
import jax.numpy as jnp
from jax import lax

C = 48
TAPS = 27
BS = 8
VOX = 512
GX = 4
GY = 4
GZ = 4
N_DP = 16
N_SPACE = 32


def draw_device_block(key, part):
    block_total = GX * GY * GZ
    crop_keys = jax.random.split(key, N_DP)

    def one_crop(crop_key):
        first_key, second_key = jax.random.split(crop_key)
        middle = jax.random.permutation(first_key, block_total - 2)[:N_SPACE - 2] + 1
        chosen = jnp.concatenate([jnp.array([0, block_total - 1], jnp.int32), middle.astype(jnp.int32)])
        return jax.random.permutation(second_key, chosen)
    return jax.vmap(one_crop)(crop_keys).astype(jnp.int32)


def touch_ends(drawn, rng, smallest, top_value):
    longest = drawn.shape.index(max(drawn.shape))
    spots = []
    for shift in (0, 1):
        where = [jax.random.randint(jax.random.fold_in(rng, axis), (), 0, length) for axis, length in enumerate(drawn.shape)]
        where[longest] = (where[longest] + shift) % drawn.shape[longest]
        spots.append(tuple(where))
    return drawn.at[spots[0]].set(smallest).at[spots[1]].set(top_value)


def levels(own_key, dims, cuts, least, top_value):
    loudness, own = 1.0, jax.random.fold_in(own_key, 6)
    for position, shards_of in cuts:
        heights = jnp.exp(jax.random.uniform(jax.random.fold_in(own, position), (shards_of,), jnp.float32, least / len(cuts), top_value / len(cuts)))
        loudness = loudness * jnp.repeat(heights, dims[position] // shards_of).reshape([-1 if axis == position else 1 for axis in range(len(dims))])
    return loudness


def centred(rng, dims, width, limit, cuts=(), held_as=jnp.bfloat16):
    entries = jax.random.normal(rng, dims, jnp.float32) * width
    if len(cuts) > 0:
        entries = levels(rng, dims, cuts, -0.22, 0.18) * entries
    return jnp.clip(entries, min=-limit, max=limit).astype(held_as)


def setup_inputs(seed: int = 0) -> dict:
    streams_of = jax.random.split(jax.random.key(seed), 7)
    return {
        "features": centred(streams_of[0], (N_DP, N_SPACE, C, VOX), 1.0, 6.0, ((0, 16), (1, 32))),
        "device_block": draw_device_block(jax.random.fold_in(streams_of[6], 71), 0),
        "conv_first": centred(streams_of[2], (C, TAPS, C), (27 * C) ** -0.5, 0.15625),
        "conv_second": centred(streams_of[3], (C, TAPS, C), (27 * C) ** -0.5, 0.15625),
        "head_weight": centred(streams_of[4], (3, C), C ** -0.5, 0.875),
        "targets": touch_ends((jax.random.randint(streams_of[5], (N_DP, N_SPACE, 3, VOX), 0, 2) < 1).astype(jnp.int32), jax.random.fold_in(streams_of[5], 1), 0, 1),
    }


def conv_volume(volume, weight, dilation):
    kernel = weight.reshape(C, 3, 3, 3, C).transpose(0, 4, 1, 2, 3)
    return lax.conv_general_dilated(volume[None], kernel, (1, 1, 1), [(dilation, dilation)] * 3, rhs_dilation=(dilation, dilation, dilation), dimension_numbers=('NCDHW', 'OIDHW', 'NCDHW'), precision=lax.Precision.HIGHEST)[0]

def elu_pair(values):
    negative = jnp.exp(jnp.minimum(values, 0.0))
    return (jnp.where(values > 0, values, negative - 1.0), jnp.where(values > 0, 1.0, negative))

def rounded(values):
    return lax.optimization_barrier(values.astype(jnp.bfloat16)).astype(jnp.float32)

def place_blocks(rows, block_ids, channels):
    grid = jnp.zeros((GX * GY * GZ, channels, BS, BS, BS), rows.dtype)
    grid = grid.at[block_ids].set(rows.reshape(N_SPACE, channels, BS, BS, BS))
    grid = grid.reshape(GX, GY, GZ, channels, BS, BS, BS).transpose(3, 0, 4, 1, 5, 2, 6)
    return grid.reshape(channels, GX * BS, GY * BS, GZ * BS)

def take_blocks(volume, block_ids, channels):
    grid = volume.reshape(channels, GX, BS, GY, BS, GZ, BS).transpose(1, 3, 5, 0, 2, 4, 6)
    return grid.reshape(GX * GY * GZ, channels, VOX)[block_ids]

def reference(features, device_block, conv_first, conv_second, head_weight, targets):
    first_w = conv_first.astype(jnp.float32)
    second_w = conv_second.astype(jnp.float32)
    head_w = head_weight.astype(jnp.float32)
    scale = 1.0 / jnp.sqrt(jnp.float32(N_DP * N_SPACE * 3 * VOX))

    def one_crop(crop_inputs):
        crop_features, block_ids, crop_targets = crop_inputs
        mask = place_blocks(jnp.ones((N_SPACE, 1, VOX), jnp.float32), block_ids, 1)
        volume = place_blocks(crop_features.astype(jnp.float32), block_ids, C)
        pre_first, pull_first = jax.vjp(lambda weight: conv_volume(volume, weight, 1), first_w)
        act_first, slope_first = elu_pair(pre_first)
        hid_first = rounded(act_first * mask)
        pre_second, pull_second = jax.vjp(lambda field, weight: conv_volume(field, weight, 2), hid_first, second_w)
        act_second, slope_second = elu_pair(pre_second)
        hid_second = rounded(act_second * mask)
        logits = jnp.einsum('jc,cxyz->jxyz', head_w, hid_second, precision=lax.Precision.HIGHEST)
        target_vol = place_blocks(crop_targets.astype(jnp.float32), block_ids, 3)
        grad_logit = rounded((jax.nn.sigmoid(logits) - target_vol) * mask * scale)
        grad_head = jnp.einsum('jxyz,cxyz->jc', grad_logit, hid_second, precision=lax.Precision.HIGHEST)
        back_second = jnp.einsum('jc,jxyz->cxyz', head_w, grad_logit, precision=lax.Precision.HIGHEST)
        grad_pre_second = rounded(back_second * slope_second * mask)
        back_first, grad_second = pull_second(grad_pre_second)
        grad_pre_first = rounded(back_first * slope_first * mask)
        grad_first = pull_first(grad_pre_first)[0]
        return (take_blocks(logits, block_ids, 3), grad_first, grad_second, grad_head)
    logit_rows, grad_first, grad_second, grad_head = lax.map(one_crop, (features, device_block, targets))
    return (logit_rows, lax.optimization_barrier(jnp.sum(grad_first, axis=0)), lax.optimization_barrier(jnp.sum(grad_second, axis=0)), lax.optimization_barrier(jnp.sum(grad_head, axis=0)))
```

```python
import jax
import jax.numpy as jnp
from jax import lax
from jax.experimental import pallas as pl
from jax.experimental.pallas import tpu as pltpu
from jax.sharding import PartitionSpec as P

BS = 8


tap_offsets = [
    (tap_index // 9 - 1, tap_index // 3 % 3 - 1, tap_index % 3 - 1) for tap_index in range(27)
]


MESH = pl.DeviceIdType.MESH


def grad_sum_kernel(g_ref, out_ref, send_buf, rs_buf, dp_buf, ag_buf, send_sem, rs_sem, dp_send, dp_sem, ag_send, ag_sem):
    dp, sp = lax.axis_index("dp"), lax.axis_index("space")
    n_dp, n_sp = dp_buf.shape[0], rs_buf.shape[0]
    rows = rs_buf.shape[1]

    barrier = pltpu.get_barrier_semaphore()

    @pl.loop(1, n_sp)
    def _(r):
        pl.semaphore_signal(barrier, inc=1, device_id=(dp, lax.rem(sp + r, n_sp)), device_id_type=MESH)

    @pl.loop(1, n_dp)
    def _(r):
        pl.semaphore_signal(barrier, inc=1, device_id=(lax.rem(dp + r, n_dp), sp), device_id_type=MESH)

    send_buf[...] = g_ref[...].reshape(send_buf.shape).astype(jnp.bfloat16)
    pl.semaphore_wait(barrier, n_sp + n_dp - 2)

    def rs_copy(r):
        peer = lax.rem(sp + r, n_sp)
        return pltpu.make_async_remote_copy(
            src_ref=send_buf.at[peer], dst_ref=rs_buf.at[r], send_sem=send_sem.at[r], recv_sem=rs_sem.at[r],
            device_id=(dp, peer), device_id_type=MESH)

    def dp_copy(r):
        peer = lax.rem(dp + r, n_dp)
        return pltpu.make_async_remote_copy(
            src_ref=dp_buf.at[0], dst_ref=dp_buf.at[r], send_sem=dp_send.at[r], recv_sem=dp_sem.at[r],
            device_id=(peer, sp), device_id_type=MESH)

    def ag_copy(r):
        peer = lax.rem(sp + r, n_sp)
        return pltpu.make_async_remote_copy(
            src_ref=ag_buf.at[0], dst_ref=ag_buf.at[r], send_sem=ag_send.at[r], recv_sem=ag_sem.at[r],
            device_id=(dp, peer), device_id_type=MESH)

    @pl.loop(1, n_sp)
    def _(r):
        rs_copy(r).start()

    def add_rs(r, total):
        rs_copy(r).wait_recv()
        return total + rs_buf[r].astype(jnp.float32)

    own = g_ref[pl.ds(pl.multiple_of(sp * rows, rows), rows), :]
    total = lax.fori_loop(1, n_sp, add_rs, own)
    dp_buf[0] = total.astype(jnp.bfloat16)

    @pl.loop(1, n_dp)
    def _(r):
        dp_copy(r).start()

    @pl.loop(1, n_dp)
    def _(r):
        dp_copy(r).wait_recv()

    def add_dp(d, total):
        return total + dp_buf[lax.rem(dp - d + n_dp, n_dp)].astype(jnp.float32)

    total = lax.fori_loop(0, n_dp, add_dp, jnp.zeros((rows, 128), jnp.float32))
    ag_buf[0] = total.astype(jnp.bfloat16)

    @pl.loop(1, n_sp)
    def _(r):
        ag_copy(r).start()

    @pl.loop(1, n_sp)
    def _(r):
        rs_copy(r).wait_send()

    @pl.loop(1, n_dp)
    def _(r):
        dp_copy(r).wait_send()

    out_ref[pl.ds(pl.multiple_of(sp * rows, rows), rows), :] = ag_buf[0].astype(jnp.float32)

    @pl.loop(1, n_sp)
    def _(r):
        ag_copy(r).wait_recv()
        source = lax.rem(sp - r + n_sp, n_sp)
        out_ref[pl.ds(pl.multiple_of(source * rows, rows), rows), :] = ag_buf[r].astype(jnp.float32)

    @pl.loop(1, n_sp)
    def _(r):
        ag_copy(r).wait_send()


def grad_sum(flat):
    n_dp, n_sp = lax.axis_size("dp"), lax.axis_size("space")
    total_rows = flat.shape[0]
    rows = total_rows // n_sp
    vmem = pl.BlockSpec(memory_space=pltpu.VMEM)
    dma = pltpu.SemaphoreType.DMA
    return pl.pallas_call(
        grad_sum_kernel,
        out_shape=jax.ShapeDtypeStruct((total_rows, 128), jnp.float32),
        in_specs=[vmem],
        out_specs=vmem,
        scratch_shapes=[
            pltpu.VMEM((n_sp, rows, 128), jnp.bfloat16),
            pltpu.VMEM((n_sp, rows, 128), jnp.bfloat16),
            pltpu.VMEM((n_dp, rows, 128), jnp.bfloat16),
            pltpu.VMEM((n_sp, rows, 128), jnp.bfloat16),
            dma((n_sp,)), dma((n_sp,)), dma((n_dp,)), dma((n_dp,)), dma((n_sp,)), dma((n_sp,)),
        ],
        compiler_params=pltpu.CompilerParams(collective_id=0, has_side_effects=True),
    )(flat)


def elu_pair(values):
    negative = jnp.exp(jnp.minimum(values, 0.0))
    return (jnp.where(values > 0, values, negative - 1.0), jnp.where(values > 0, 1.0, negative))


def neighbor_tables(device_block):
    space_count = lax.axis_size("space")
    depth_z = space_count // 8
    self_index = lax.axis_index("space")
    blocks = device_block[0]
    coords = jnp.stack([blocks // (4 * depth_z), blocks // depth_z % 4, blocks % depth_z])
    own_coords = lax.dynamic_index_in_dim(coords, self_index, 1, keepdims=False)
    offsets = jnp.array(tap_offsets, jnp.int32)
    limits = jnp.array([4, 4, depth_z], jnp.int32)
    wanted = own_coords[None, :] + offsets
    inside = jnp.all((wanted >= 0) & (wanted < limits[None, :]), axis=1) & (jnp.arange(27) != 13)
    wanted_id = (wanted[:, 0] * 4 + wanted[:, 1]) * depth_z + wanted[:, 2]
    matches = (blocks[None, :] == wanted_id[:, None]) & inside[:, None]
    devices = jnp.arange(space_count, dtype=jnp.int32)
    owner_row = jnp.sum(jnp.where(matches, devices[None, :], 0), axis=1)
    present = jnp.any(matches, axis=1)
    relative = coords - own_coords[:, None]
    adjacent = jnp.all(jnp.abs(relative) <= 1, axis=0) & (devices != self_index)
    send_tap = jnp.where(
        adjacent, (relative[0] + 1) * 9 + (relative[1] + 1) * 3 + relative[2] + 1, 13
    )
    return (owner_row, present, send_tap)


def region_slice(block_data, offset, depth_cells):
    span_list = []
    for step_value in offset:
        if step_value == 1:
            span_list.append(slice(BS - depth_cells, BS))
        elif step_value == -1:
            span_list.append(slice(0, depth_cells))
        else:
            span_list.append(slice(0, BS))
    return block_data[:, span_list[0], span_list[1], span_list[2]]


def surround(block_data, depth_cells, tables):
    owner_row, present, send_tap = tables
    channels = block_data.shape[0]
    length = depth_cells * BS * BS
    pieces = []
    for tap_index in range(27):
        if tap_index == 13:
            pieces.append(jnp.zeros((channels, length), block_data.dtype))
        else:
            region = region_slice(block_data, tap_offsets[tap_index], depth_cells).reshape(
                channels, -1
            )
            pieces.append(jnp.pad(region, ((0, 0), (0, length - region.shape[1]))))
    outgoing = jnp.stack(pieces)
    sending = outgoing[send_tap]
    by_source = lax.all_to_all(sending, "space", split_axis=0, concat_axis=0, tiled=True)
    incoming = jnp.where(
        present[:, None, None], by_source[owner_row], jnp.zeros((), block_data.dtype)
    )
    rows_x = []
    for step_x in range(3):
        rows_y = []
        for step_y in range(3):
            rows_z = []
            for step_z in range(3):
                tap_index = step_x * 9 + step_y * 3 + step_z
                if tap_index == 13:
                    rows_z.append(block_data)
                else:
                    extent_list = [
                        BS if step_value == 1 else depth_cells
                        for step_value in (step_x, step_y, step_z)
                    ]
                    count_cells = extent_list[0] * extent_list[1] * extent_list[2]
                    rows_z.append(
                        incoming[tap_index][:, :count_cells].reshape(
                            channels, extent_list[0], extent_list[1], extent_list[2]
                        )
                    )
            rows_y.append(jnp.concatenate(rows_z, axis=3))
        rows_x.append(jnp.concatenate(rows_y, axis=2))
    return jnp.concatenate(rows_x, axis=1)


def conv_padded(padded, kernel, dilation):
    result = lax.conv_general_dilated(
        padded[None],
        kernel,
        (1, 1, 1),
        "VALID",
        rhs_dilation=(dilation, dilation, dilation),
        dimension_numbers=("NCDHW", "OIDHW", "NCDHW"),
        preferred_element_type=jnp.float32,
    )
    return result[0].reshape(kernel.shape[0], BS * BS * BS)


def kernel_grad(padded, grad_rows, dilation):
    channels = padded.shape[0]
    outputs = grad_rows.shape[0]
    grad_block = grad_rows.reshape(outputs, 1, BS, BS, BS)
    result = lax.conv_general_dilated(
        padded[None],
        grad_block,
        (dilation, dilation, dilation),
        "VALID",
        dimension_numbers=("CNDHW", "OIDHW", "NCDHW"),
        preferred_element_type=jnp.float32,
    )
    return result.reshape(channels, outputs, 27).transpose(1, 2, 0)


def on_device(features, device_block, conv_first, conv_second, head_weight, targets):
    channels = features.shape[2]
    tables = neighbor_tables(device_block)
    kernel_first = conv_first.reshape(channels, 3, 3, 3, channels).transpose(0, 4, 1, 2, 3)
    kernel_second = conv_second.reshape(channels, 3, 3, 3, channels).transpose(0, 4, 1, 2, 3)
    block_in = features[0, 0].reshape(channels, BS, BS, BS)
    padded_in = surround(block_in, 1, tables)
    pre_first = conv_padded(padded_in, kernel_first, 1)
    act_first, slope_first = elu_pair(pre_first)
    hid_first = act_first.astype(jnp.bfloat16)
    padded_first = surround(hid_first.reshape(channels, BS, BS, BS), 2, tables)
    pre_second = conv_padded(padded_first, kernel_second, 2)
    act_second, slope_second = elu_pair(pre_second)
    hid_second = act_second.astype(jnp.bfloat16)
    logits = jnp.dot(head_weight, hid_second, preferred_element_type=jnp.float32)
    scale = (lax.axis_size("dp") * lax.axis_size("space") * 3 * BS * BS * BS) ** (-0.5)
    grad_logit = ((jax.nn.sigmoid(logits) - targets[0, 0].astype(jnp.float32)) * scale).astype(
        jnp.bfloat16
    )
    grad_head = lax.dot_general(
        grad_logit, hid_second, (((1,), (1,)), ((), ())), preferred_element_type=jnp.float32
    )
    back_second = lax.dot_general(
        head_weight, grad_logit, (((0,), (0,)), ((), ())), preferred_element_type=jnp.float32
    )
    grad_pre_second = (back_second * slope_second).astype(jnp.bfloat16)
    grad_second = kernel_grad(padded_first, grad_pre_second, 2)
    padded_grad = surround(grad_pre_second.reshape(channels, BS, BS, BS), 2, tables)
    kernel_back = jnp.transpose(kernel_second[:, :, ::-1, ::-1, ::-1], (1, 0, 2, 3, 4))
    back_first = conv_padded(padded_grad, kernel_back, 2)
    grad_pre_first = (back_first * slope_first).astype(jnp.bfloat16)
    grad_first = kernel_grad(padded_in, grad_pre_first, 1)
    flat_grads = jnp.concatenate(
        [grad_first.reshape(-1), grad_second.reshape(-1), grad_head.reshape(-1)]
    )
    full_len = flat_grads.shape[0]
    chunk = 16 * 128 * lax.axis_size("space")
    padded_len = -(-full_len // chunk) * chunk
    flat_grads = jnp.pad(flat_grads, (0, padded_len - full_len))
    all_grads = grad_sum(flat_grads.reshape(-1, 128)).reshape(-1)
    kernel_len = 27 * channels * channels
    grad_first = all_grads[:kernel_len].reshape(channels, 27, channels)
    grad_second = all_grads[kernel_len : 2 * kernel_len].reshape(channels, 27, channels)
    grad_head = all_grads[2 * kernel_len : 2 * kernel_len + 3 * channels].reshape(3, channels)
    return (logits[None, None], grad_first, grad_second, grad_head)


def solution(mesh):
    in_specs = (
        P("dp", "space", None, None),
        P("dp", None),
        P(),
        P(),
        P(),
        P("dp", "space", None, None),
    )
    out_specs = (P("dp", "space", None, None), P(), P(), P())
    return jax.shard_map(
        on_device, mesh=mesh, in_specs=in_specs, out_specs=out_specs, check_vma=False
    )
```

```python
import functools
import jax
import jax.numpy as jnp
from jax import lax
from jax.experimental import pallas as pl
from jax.experimental.pallas import tpu as pltpu
from jax.sharding import PartitionSpec as P

BF = jnp.bfloat16
F32 = jnp.float32
C = 48
LANES = 256
NT = (((1,), (1,)), ((), ()))


def dot32(a, b):
    return jnp.dot(a, b, preferred_element_type=F32)


def elu_pair(values):
    negative = jnp.exp(jnp.minimum(values, 0.0))
    return (jnp.where(values > 0, values, negative - 1.0), jnp.where(values > 0, 1.0, negative))


def plane(index):
    start = index * LANES
    return pl.ds(start if isinstance(index, int) else pl.multiple_of(start, LANES), LANES)


def compute_kernel(scale, ids_ref, got_ref, w1_ref, w2_ref, wb_ref, head_ref, head_t_ref,
                   logits_ref, grads_ref,
                   table, near, near_t, wide1, out1, pre1, wide2, out2, wide_b, out_b, lhs2, lhs1, want, mask_ref,
                   head_acc):
    me = lax.axis_index("space")

    @pl.loop(0, 64)
    def _(i):
        table[i] = -1

    @pl.loop(0, 32)
    def _(j):
        table[ids_ref[0, j]] = j

    own = ids_ref[0, me]
    ox, oy, oz = own // 16, own // 4 % 4, own % 4
    slots, present = [], []
    for t in range(27):
        x, y, z = ox + t // 9 - 1, oy + t // 3 % 3 - 1, oz + t % 3 - 1
        inside = (x >= 0) & (x < 4) & (y >= 0) & (y < 4) & (z >= 0) & (z < 4)
        found = table[jnp.where(inside, (x * 4 + y) * 4 + z, own)]
        ok = inside & (found >= 0)
        slots.append(jnp.where(ok, found, me))
        present.append(jnp.where(ok, 1.0, 0.0).astype(F32))

    low_half = lax.broadcasted_iota(jnp.int32, (C, 128), 1) < 64

    def tiles_of(bx, row, rows):
        return [
            (got_ref[slots[bx * 9 + j], row:row + rows, :].astype(F32) * present[bx * 9 + j]).astype(BF)
            for j in range(9)
        ]

    def face_tiles(tiles, half):
        rows = tiles[0].shape[0]
        keep = low_half[:rows]
        flip = lambda v: pltpu.roll(v, 64, 1)
        for k in range(5):
            low = tiles[2 * k] if half == 0 else flip(tiles[2 * k])
            if k == 4:
                high = jnp.zeros_like(low)
            else:
                high = tiles[2 * k + 1] if half == 1 else flip(tiles[2 * k + 1])
            yield k, jnp.where(keep, low, high)

    for bx in range(3):
        for pair in range(4):
            spots = [(half, bx * 8 + pair * 2 + half - 3) for half in range(2)]
            spots = [(half, at) for half, at in spots if 0 <= at < 18]
            if not spots:
                continue
            tiles = tiles_of(bx, pair * C, C)
            for half, at in spots:
                for k, value in face_tiles(tiles, half):
                    near[at * C:(at + 1) * C, k * 128:(k + 1) * 128] = value
        tiles = tiles_of(bx, 4 * C, 16)
        for half in range(2):
            for k, value in face_tiles(tiles, half):
                near_t[(bx * 2 + half) * 16:(bx * 2 + half + 1) * 16, k * 128:(k + 1) * 128] = value

    lane = lax.broadcasted_iota(jnp.int32, (1, LANES), 1)
    face_row = lax.broadcasted_iota(jnp.int32, (640, LANES), 0)

    def select_of(b, c):
        y = (lane >> 4) + (b + 3)
        z = (lane & 15) + (c + 3)
        source = ((y >> 3) * 3 + (z >> 3)) * 64 + (y & 7) * 8 + (z & 7)
        return jnp.where(face_row == source, 1.0, 0.0).astype(BF)

    @pl.loop(0, 9)
    def _(bc):
        picked = dot32(near[...], select_of(bc // 3, bc % 3)).astype(BF)
        rows = pl.ds(pl.multiple_of(bc * C, 16), C)
        for at in range(18):
            wide1[rows, plane(at)] = picked[at * C:(at + 1) * C]

    picked_t = dot32(near_t[...], select_of(1, 1))
    want[...] = jnp.zeros_like(want)
    for xo in range(2, 14):
        bx, x = (xo + 4) // 8, (xo + 4) % 8
        row = (bx * 2 + x % 2) * 16 + (x // 2) * 4
        want[xo - 2, 0:3, :] = picked_t[row:row + 3]

    y, z = lane >> 4, lane & 15
    region = ((y + 4) >> 3) * 3 + ((z + 4) >> 3)
    inner = jnp.where((y >= 2) & (y < 14) & (z >= 2) & (z < 14), 1.0, 0.0)
    own_lane = jnp.where((y >= 4) & (y < 12) & (z >= 4) & (z < 12), 1.0, 0.0)
    for bx in range(3):
        row = jnp.zeros((1, LANES), F32)
        for j in range(9):
            row = jnp.where(region == j, present[bx * 9 + j], row)
        mask_ref[bx, 0:1, :] = row
        mask_ref[bx, 1:2, :] = row * inner

    def region_of(xo):
        return jnp.where(xo >= 12, 2, jnp.where(xo >= 4, 1, 0))

    out1[...] = dot32(w1_ref[...], wide1[...])

    @pl.loop(0, 16)
    def _(xo):
        pre = out1[0:C, plane(xo)] + out1[C:2 * C, plane(xo + 1)] + out1[2 * C:3 * C, plane(xo + 2)]
        pre1[xo] = pre
        act, _slope = elu_pair(pre)
        hid = (act * mask_ref[region_of(xo), 0:1, :]).astype(BF)
        for bc in range(9):
            shift = -(32 * (bc // 3 - 1) + 2 * (bc % 3 - 1)) % LANES
            wide2[bc * C:(bc + 1) * C, plane(xo)] = pltpu.roll(hid, shift, 1) if shift else hid

    out2[...] = dot32(w2_ref[...], wide2[...])
    lhs2[...] = jnp.zeros_like(lhs2)
    lhs1[...] = jnp.zeros_like(lhs1)
    head_acc[...] = jnp.zeros_like(head_acc)

    def second(xo, is_own):
        pre = out2[0:C, plane(xo - 2)] + out2[C:2 * C, plane(xo)] + out2[2 * C:3 * C, plane(xo + 2)]
        act, slope = elu_pair(pre)
        mask = mask_ref[region_of(xo), 1:2, :]
        hid = (act * mask).astype(BF)
        logits = dot32(head_ref[...], hid)
        grad_logit = ((jax.nn.sigmoid(logits) - want[xo - 2]) * mask * scale).astype(BF)
        back = dot32(head_t_ref[...], grad_logit)
        grad_pre = (back * slope * mask).astype(BF)
        for bc in range(9):
            shift = (32 * (bc // 3 - 1) + 2 * (bc % 3 - 1)) % LANES
            wide_b[bc * C:(bc + 1) * C, plane(xo - 2)] = pltpu.roll(grad_pre, shift, 1) if shift else grad_pre
        if is_own:
            logits_ref[xo - 4] = logits[0:8]
            own_logit = (grad_logit.astype(F32) * own_lane).astype(BF)
            head_acc[...] += lax.dot_general(own_logit, hid, NT, preferred_element_type=F32)
            own_pre = (grad_pre.astype(F32) * own_lane).astype(BF)
            for a in range(3):
                lhs2[a * C:(a + 1) * C, plane(xo + 2 * a - 4)] = own_pre

    @pl.loop(0, 8)
    def _(i):
        second(i + 4, True)

    @pl.loop(0, 4)
    def _(i):
        second(jnp.where(i < 2, i + 2, i + 10), False)

    grads_ref[3 * C:6 * C, 0:9 * C] = lax.dot_general(
        lhs2[...], wide2[:, 2 * LANES:14 * LANES], NT, preferred_element_type=F32)
    out_b[...] = dot32(wb_ref[...], wide_b[...])

    @pl.loop(4, 12)
    def _(q):
        back = out_b[0:C, plane(q)] + out_b[C:2 * C, plane(q - 2)] + out_b[2 * C:3 * C, plane(q - 4)]
        _act, slope = elu_pair(pre1[q])
        grad_pre = (back * slope * own_lane).astype(BF)
        for a in range(3):
            lhs1[a * C:(a + 1) * C, plane(q + a - 4)] = grad_pre

    grads_ref[0:3 * C, 0:9 * C] = lax.dot_general(
        lhs1[...], wide1[:, 4 * LANES:14 * LANES], NT, preferred_element_type=F32)
    grads_ref[:, 9 * C:512] = jnp.zeros((6 * C, 512 - 9 * C), F32)
    grads_ref[0:16, 9 * C:10 * C] = head_acc[...]


def compute_block(ids, got, w1, w2, wb, head, head_t, scale):
    vmem = pl.BlockSpec(memory_space=pltpu.VMEM)
    v = pltpu.VMEM
    return pl.pallas_call(
        functools.partial(compute_kernel, scale),
        out_shape=(jax.ShapeDtypeStruct((8, 8, LANES), F32), jax.ShapeDtypeStruct((6 * C, 512), F32)),
        in_specs=[pl.BlockSpec(memory_space=pltpu.SMEM)] + [vmem] * 6,
        out_specs=(vmem, vmem),
        scratch_shapes=[
            pltpu.SMEM((64,), jnp.int32),
            v((18 * C, 640), BF), v((96, 640), BF),
            v((9 * C, 18 * LANES), BF), v((3 * C, 18 * LANES), F32), v((16, C, LANES), F32),
            v((9 * C, 16 * LANES), BF), v((3 * C, 16 * LANES), F32),
            v((9 * C, 12 * LANES), BF), v((3 * C, 12 * LANES), F32),
            v((3 * C, 12 * LANES), BF), v((3 * C, 10 * LANES), BF),
            v((12, 16, LANES), F32), v((3, 8, LANES), F32), v((16, C), F32),
        ],
        compiler_params=pltpu.CompilerParams(vmem_limit_bytes=60 * 1024 * 1024),
    )(ids, got, w1, w2, wb, head, head_t)


def stacked(kernel):
    return kernel.reshape(C, 3, 9 * C).transpose(1, 0, 2).reshape(3 * C, 9 * C)


def stacked_back(kernel):
    return kernel.reshape(C, 3, 9, C).transpose(1, 3, 2, 0).reshape(3 * C, 9 * C)


def payload(features, targets):
    feats = features.reshape(C, 4, 128).transpose(1, 0, 2).reshape(4 * C, 128)
    wants = jnp.pad(targets.astype(BF).reshape(3, 4, 128).transpose(1, 0, 2), ((0, 0), (0, 1), (0, 0)))
    return jnp.concatenate([feats, wants.reshape(16, 128)], axis=0)


MESH = pl.DeviceIdType.MESH
N_Z, N_X = 8, 4
SPLIT = 96


def gather_kernel(own_ref, got_ref, send_sem, recv_sem):
    dp, sp = lax.axis_index("dp"), lax.axis_index("space")
    z, x = lax.div(sp, N_X), lax.rem(sp, N_X)

    def at(dz, dx):
        return lax.rem(z + dz + N_Z, N_Z) * N_X + lax.rem(x + dx + N_X, N_X)

    near_by = [(1, 0), (-1, 0), (0, 1), (0, -1), (0, 2)]
    barrier = pltpu.get_barrier_semaphore()
    for dz, dx in near_by:
        pl.semaphore_signal(barrier, inc=1, device_id=(dp, at(dz, dx)), device_id_type=MESH)
    pl.semaphore_wait(barrier, len(near_by))

    rows = [pl.ds(0, SPLIT), pl.ds(SPLIT, own_ref.shape[0] - SPLIT)]
    sent = []

    def copy(half, dz, dx, to, number):
        slot = at(dz, dx)
        source = own_ref.at[rows[half]] if (dz, dx) == (0, 0) else got_ref.at[slot, rows[half]]
        return pltpu.make_async_remote_copy(
            src_ref=source, dst_ref=got_ref.at[slot, rows[half]], send_sem=send_sem.at[number],
            recv_sem=recv_sem.at[half, slot], device_id=(dp, at(*to)), device_id_type=MESH)

    def send(half, dz, dx, to):
        one = copy(half, dz, dx, to, len(sent))
        one.start()
        sent.append(one)

    arrived = set()

    def await_block(half, dz, dx):
        if (half, dz, dx) not in arrived and (dz, dx) != (0, 0):
            slot = at(dz, dx)
            pltpu.make_async_remote_copy(
                src_ref=own_ref.at[rows[half]], dst_ref=got_ref.at[slot, rows[half]], send_sem=send_sem.at[0],
                recv_sem=recv_sem.at[half, slot], device_id=(dp, at(0, 1)), device_id_type=MESH).wait_recv()
            arrived.add((half, dz, dx))

    def reach(way, dx):
        return 4 if (way == 1) == (dx in (0, 1)) else 3

    for way in (1, -1):
        send(1, 0, 0, (way, 0))
    for dx in (1, -1, 2):
        send(0, 0, 0, (0, dx))
    for way in (1, -1):
        send(0, 0, 0, (way, 0))
    for dx in (1, -1, 2):
        send(1, 0, 0, (0, dx))
    got_ref[sp] = own_ref[...]

    for k in range(4):
        for dx in (0, 1, -1, 2):
            for way in (1, -1):
                if (k, dx) != (0, 0) and k < reach(way, dx):
                    await_block(0, -way * k, dx)
                    send(0, -way * k, dx, (way, 0))
        for way in (1, -1):
            far = k + 1
            if far <= reach(way, 0):
                await_block(1, -way * far, 0)
                if far < reach(way, 0):
                    send(1, -way * far, 0, (way, 0))
                for dx in (1, -1, 2):
                    send(1, -way * far, 0, (0, dx))

    for half in range(2):
        for dx in (0, 1, -1, 2):
            column = dx if half == 0 else 0
            for way in (1, -1):
                for k in range(reach(way, column) + 1):
                    await_block(half, -way * k, dx)
    for one in sent:
        one.wait_send()


def gather_blocks(own):
    vmem = pl.BlockSpec(memory_space=pltpu.VMEM)
    return pl.pallas_call(
        gather_kernel,
        out_shape=jax.ShapeDtypeStruct((N_Z * N_X, *own.shape), own.dtype),
        in_specs=[vmem],
        out_specs=vmem,
        scratch_shapes=[pltpu.SemaphoreType.DMA((64,)), pltpu.SemaphoreType.DMA((2, N_Z * N_X))],
        compiler_params=pltpu.CompilerParams(collective_id=1, has_side_effects=True),
    )(own)


def grad_sum_kernel(g_ref, out_ref, send_buf, rs_buf, dp_buf, ag_buf, send_sem, rs_sem, dp_send, dp_sem, ag_send, ag_sem):
    dp, sp = lax.axis_index("dp"), lax.axis_index("space")
    n_dp, n_sp = dp_buf.shape[0], rs_buf.shape[0]
    rows = rs_buf.shape[1]

    barrier = pltpu.get_barrier_semaphore()

    @pl.loop(1, n_sp)
    def _(r):
        pl.semaphore_signal(barrier, inc=1, device_id=(dp, lax.rem(sp + r, n_sp)), device_id_type=MESH)

    @pl.loop(1, n_dp)
    def _(r):
        pl.semaphore_signal(barrier, inc=1, device_id=(lax.rem(dp + r, n_dp), sp), device_id_type=MESH)

    send_buf[...] = g_ref[...].astype(jnp.bfloat16)
    pl.semaphore_wait(barrier, n_sp + n_dp - 2)

    def rs_copy(r):
        peer = lax.rem(sp + r, n_sp)
        return pltpu.make_async_remote_copy(
            src_ref=send_buf.at[peer], dst_ref=rs_buf.at[r], send_sem=send_sem.at[r], recv_sem=rs_sem.at[r],
            device_id=(dp, peer), device_id_type=MESH)

    def dp_copy(r):
        peer = lax.rem(dp + r, n_dp)
        return pltpu.make_async_remote_copy(
            src_ref=dp_buf.at[0], dst_ref=dp_buf.at[r], send_sem=dp_send.at[r], recv_sem=dp_sem.at[r],
            device_id=(peer, sp), device_id_type=MESH)

    def ag_copy(r):
        peer = lax.rem(sp + r, n_sp)
        return pltpu.make_async_remote_copy(
            src_ref=ag_buf.at[0], dst_ref=ag_buf.at[r], send_sem=ag_send.at[r], recv_sem=ag_sem.at[r],
            device_id=(dp, peer), device_id_type=MESH)

    @pl.loop(1, n_sp)
    def _(r):
        rs_copy(r).start()

    def add_rs(r, total):
        rs_copy(r).wait_recv()
        return total + rs_buf[r].astype(jnp.float32)

    own = g_ref[sp]
    total = lax.fori_loop(1, n_sp, add_rs, own)
    dp_buf[0] = total.astype(jnp.bfloat16)

    @pl.loop(1, n_dp)
    def _(r):
        dp_copy(r).start()

    @pl.loop(1, n_dp)
    def _(r):
        dp_copy(r).wait_recv()

    def add_dp(d, total):
        return total + dp_buf[lax.rem(dp - d + n_dp, n_dp)].astype(jnp.float32)

    total = lax.fori_loop(0, n_dp, add_dp, jnp.zeros((rows, 128), jnp.float32))
    ag_buf[0] = total.astype(jnp.bfloat16)

    @pl.loop(1, n_sp)
    def _(r):
        ag_copy(r).start()

    @pl.loop(1, n_sp)
    def _(r):
        rs_copy(r).wait_send()

    @pl.loop(1, n_dp)
    def _(r):
        dp_copy(r).wait_send()

    out_ref[sp] = ag_buf[0].astype(jnp.float32)

    @pl.loop(1, n_sp)
    def _(r):
        ag_copy(r).wait_recv()
        source = lax.rem(sp - r + n_sp, n_sp)
        out_ref[source] = ag_buf[r].astype(jnp.float32)

    @pl.loop(1, n_sp)
    def _(r):
        ag_copy(r).wait_send()


def grad_sum(flat):
    n_dp, n_sp = lax.axis_size("dp"), lax.axis_size("space")
    rows = flat.shape[1]
    vmem = pl.BlockSpec(memory_space=pltpu.VMEM)
    dma = pltpu.SemaphoreType.DMA
    return pl.pallas_call(
        grad_sum_kernel,
        out_shape=jax.ShapeDtypeStruct(flat.shape, jnp.float32),
        in_specs=[vmem],
        out_specs=vmem,
        scratch_shapes=[
            pltpu.VMEM((n_sp, rows, 128), jnp.bfloat16),
            pltpu.VMEM((n_sp, rows, 128), jnp.bfloat16),
            pltpu.VMEM((n_dp, rows, 128), jnp.bfloat16),
            pltpu.VMEM((n_sp, rows, 128), jnp.bfloat16),
            dma((n_sp,)), dma((n_sp,)), dma((n_dp,)), dma((n_dp,)), dma((n_sp,)), dma((n_sp,)),
        ],
        compiler_params=pltpu.CompilerParams(collective_id=0, has_side_effects=True),
    )(flat)


def on_device(features, device_block, conv_first, conv_second, head_weight, targets):
    n_dp, n_sp = lax.axis_size("dp"), lax.axis_size("space")
    scale = (n_dp * n_sp * 3 * 512) ** (-0.5)
    got = gather_blocks(payload(features[0, 0], targets[0, 0]))
    head = jnp.pad(head_weight, ((0, 13), (0, 0)))
    logits, grads = compute_block(
        device_block, got, stacked(conv_first), stacked(conv_second), stacked_back(conv_second), head, head.T, scale)
    logits = logits[:, :3].reshape(8, 3, 16, 16)[:, :, 4:12, 4:12].transpose(1, 0, 2, 3).reshape(3, 512)
    tiles = grads.reshape(6, C, 4, 128).transpose(0, 2, 1, 3).reshape(24, C, 128)
    tiles = grad_sum(jnp.pad(tiles, ((0, n_sp - 24), (0, 0), (0, 0))))[:24]
    grads = tiles.reshape(2, 3, 4, C, 128).transpose(0, 3, 1, 2, 4).reshape(2, C, 3, 512)
    kernels = grads[..., :9 * C].reshape(2, C, 27, C)
    return (logits[None, None], kernels[0], kernels[1], grads[0, :3, 0, 9 * C:10 * C])


def solution(mesh):
    in_specs = (
        P("dp", "space", None, None),
        P("dp", None),
        P(),
        P(),
        P(),
        P("dp", "space", None, None),
    )
    out_specs = (P("dp", "space", None, None), P(), P(), P())
    return jax.shard_map(
        on_device, mesh=mesh, in_specs=in_specs, out_specs=out_specs, check_vma=False
    )
```

```python
import functools
import jax
import jax.numpy as jnp
from jax import lax
from jax.experimental import pallas as pl
from jax.experimental.pallas import tpu as pltpu
from jax.sharding import PartitionSpec as P

BF = jnp.bfloat16
F32 = jnp.float32
C = 48
LANES = 256
NT = (((1,), (1,)), ((), ()))
TN = (((0,), (0,)), ((), ()))


def dot32(a, b):
    return jnp.dot(a, b, preferred_element_type=F32)


def elu_pair(values):
    negative = jnp.exp(jnp.minimum(values, 0.0))
    return (jnp.where(values > 0, values, negative - 1.0), jnp.where(values > 0, 1.0, negative))


def plane(index):
    start = index * LANES
    return pl.ds(start if isinstance(index, int) else pl.multiple_of(start, LANES), LANES)


def pack_grads(grads_ref, part, grads, head):
    for group in range(9):
        rows = grads[group * 16:(group + 1) * 16]
        for col in range(3):
            grads_ref[part, group * 3 + col] = rows[:, col * 128:(col + 1) * 128]
        grads_ref[part, 27 + group // 2, :, 64 * (group % 2):64 * (group % 2) + C] = rows[:, 384:9 * C]
    grads_ref[part, 31, :, 64:64 + C] = head


def compute_kernel(scale, ids_ref, got_ref, k1_ref, k2_ref, head_in_ref,
                   logits_ref, grads_ref,
                   table, near, near_t, wide1, out1, pre1, wide2, out2, wide_b, out_b, lhs2, lhs1, want, mask_ref,
                   head_acc, w1_ref, w2_ref, wb_ref, head_ref, raw_logits):
    me = lax.axis_index("space")

    for t in range(27):
        a, bc = t // 9, t % 9
        w1_ref[a * C:(a + 1) * C, bc * C:(bc + 1) * C] = k1_ref[t]
        w2_ref[a * C:(a + 1) * C, bc * C:(bc + 1) * C] = k2_ref[t]
        wb_ref[bc * C:(bc + 1) * C, a * C:(a + 1) * C] = k2_ref[t]
    head_ref[...] = jnp.zeros_like(head_ref)
    head_ref[0:3, :] = head_in_ref[...].astype(F32)
    head = head_ref[...].astype(BF)
    head_t = head_ref[...].T.astype(BF)

    @pl.loop(0, 64)
    def _(i):
        table[i] = -1

    @pl.loop(0, 32)
    def _(j):
        table[ids_ref[0, j]] = j

    own = ids_ref[0, me]
    ox, oy, oz = own // 16, own // 4 % 4, own % 4
    slots, present = [], []
    for t in range(27):
        x, y, z = ox + t // 9 - 1, oy + t // 3 % 3 - 1, oz + t % 3 - 1
        inside = (x >= 0) & (x < 4) & (y >= 0) & (y < 4) & (z >= 0) & (z < 4)
        found = table[jnp.where(inside, (x * 4 + y) * 4 + z, own)]
        ok = inside & (found >= 0)
        slots.append(jnp.where(ok, found, me))
        present.append(jnp.where(ok, 1.0, 0.0).astype(F32))

    low_half = lax.broadcasted_iota(jnp.int32, (C, 128), 1) < 64

    def tiles_of(bx, row, rows):
        return [
            (got_ref[slots[bx * 9 + j], row:row + rows, :].astype(F32) * present[bx * 9 + j]).astype(BF)
            for j in range(9)
        ]

    def face_tiles(tiles, half):
        rows = tiles[0].shape[0]
        keep = low_half[:rows]
        flip = lambda v: pltpu.roll(v, 64, 1)
        for k in range(5):
            low = tiles[2 * k] if half == 0 else flip(tiles[2 * k])
            if k == 4:
                high = jnp.zeros_like(low)
            else:
                high = tiles[2 * k + 1] if half == 1 else flip(tiles[2 * k + 1])
            yield k, jnp.where(keep, low, high)

    for bx in range(3):
        for pair in range(4):
            spots = [(half, bx * 8 + pair * 2 + half - 3) for half in range(2)]
            spots = [(half, at) for half, at in spots if 0 <= at < 18]
            if not spots:
                continue
            tiles = tiles_of(bx, pair * C, C)
            for half, at in spots:
                for k, value in face_tiles(tiles, half):
                    near[at * C:(at + 1) * C, k * 128:(k + 1) * 128] = value
        tiles = tiles_of(bx, 4 * C, 16)
        for half in range(2):
            for k, value in face_tiles(tiles, half):
                near_t[(bx * 2 + half) * 16:(bx * 2 + half + 1) * 16, k * 128:(k + 1) * 128] = value

    lane = lax.broadcasted_iota(jnp.int32, (1, LANES), 1)
    face_row = lax.broadcasted_iota(jnp.int32, (640, LANES), 0)

    def select_of(b, c):
        y = (lane >> 4) + (b + 3)
        z = (lane & 15) + (c + 3)
        source = ((y >> 3) * 3 + (z >> 3)) * 64 + (y & 7) * 8 + (z & 7)
        return jnp.where(face_row == source, 1.0, 0.0).astype(BF)

    @pl.loop(0, 9)
    def _(bc):
        picked = dot32(near[...], select_of(bc // 3, bc % 3)).astype(BF)
        rows = pl.ds(pl.multiple_of(bc * C, 16), C)
        for at in range(18):
            wide1[rows, plane(at)] = picked[at * C:(at + 1) * C]

    picked_t = dot32(near_t[...], select_of(1, 1))
    want[...] = jnp.zeros_like(want)
    for xo in range(2, 14):
        bx, x = (xo + 4) // 8, (xo + 4) % 8
        row = (bx * 2 + x % 2) * 16 + (x // 2) * 4
        want[xo - 2, 0:3, :] = picked_t[row:row + 3]

    y, z = lane >> 4, lane & 15
    region = ((y + 4) >> 3) * 3 + ((z + 4) >> 3)
    inner = jnp.where((y >= 2) & (y < 14) & (z >= 2) & (z < 14), 1.0, 0.0)
    own_lane = jnp.where((y >= 4) & (y < 12) & (z >= 4) & (z < 12), 1.0, 0.0)
    for bx in range(3):
        row = jnp.zeros((1, LANES), F32)
        for j in range(9):
            row = jnp.where(region == j, present[bx * 9 + j], row)
        mask_ref[bx, 0:1, :] = row
        mask_ref[bx, 1:2, :] = row * inner

    def region_of(xo):
        return jnp.where(xo >= 12, 2, jnp.where(xo >= 4, 1, 0))

    out1[...] = dot32(w1_ref[...], wide1[...])

    @pl.loop(0, 16)
    def _(xo):
        pre = out1[0:C, plane(xo)] + out1[C:2 * C, plane(xo + 1)] + out1[2 * C:3 * C, plane(xo + 2)]
        pre1[xo] = pre
        act, _slope = elu_pair(pre)
        hid = (act * mask_ref[region_of(xo), 0:1, :]).astype(BF)
        for bc in range(9):
            shift = -(32 * (bc // 3 - 1) + 2 * (bc % 3 - 1)) % LANES
            wide2[bc * C:(bc + 1) * C, plane(xo)] = pltpu.roll(hid, shift, 1) if shift else hid

    out2[...] = dot32(w2_ref[...], wide2[...])
    lhs2[...] = jnp.zeros_like(lhs2)
    lhs1[...] = jnp.zeros_like(lhs1)
    head_acc[...] = jnp.zeros_like(head_acc)

    def second(xo, is_own):
        pre = out2[0:C, plane(xo - 2)] + out2[C:2 * C, plane(xo)] + out2[2 * C:3 * C, plane(xo + 2)]
        act, slope = elu_pair(pre)
        mask = mask_ref[region_of(xo), 1:2, :]
        hid = (act * mask).astype(BF)
        logits = dot32(head, hid)
        grad_logit = ((jax.nn.sigmoid(logits) - want[xo - 2]) * mask * scale).astype(BF)
        back = dot32(head_t, grad_logit)
        grad_pre = (back * slope * mask).astype(BF)
        for bc in range(9):
            shift = (32 * (bc // 3 - 1) + 2 * (bc % 3 - 1)) % LANES
            wide_b[bc * C:(bc + 1) * C, plane(xo - 2)] = pltpu.roll(grad_pre, shift, 1) if shift else grad_pre
        if is_own:
            raw_logits[pl.ds(pl.multiple_of((xo - 4) * 8, 8), 8), :] = logits[0:8]
            own_logit = (grad_logit.astype(F32) * own_lane).astype(BF)
            head_acc[...] += lax.dot_general(own_logit, hid, NT, preferred_element_type=F32)
            own_pre = (grad_pre.astype(F32) * own_lane).astype(BF)
            for a in range(3):
                lhs2[a * C:(a + 1) * C, plane(xo + 2 * a - 4)] = own_pre

    @pl.loop(0, 8)
    def _(i):
        second(i + 4, True)

    @pl.loop(0, 4)
    def _(i):
        second(jnp.where(i < 2, i + 2, i + 10), False)

    grads_ref[:, 27:32] = jnp.zeros((2, 5, 16, 128), F32)
    pack_grads(grads_ref, 1, lax.dot_general(
        lhs2[...], wide2[:, 2 * LANES:14 * LANES], NT, preferred_element_type=F32), jnp.zeros((16, C), F32))
    out_b[...] = lax.dot_general(wb_ref[...], wide_b[...], TN, preferred_element_type=F32)

    @pl.loop(4, 12)
    def _(q):
        back = out_b[0:C, plane(q)] + out_b[C:2 * C, plane(q - 2)] + out_b[2 * C:3 * C, plane(q - 4)]
        _act, slope = elu_pair(pre1[q])
        grad_pre = (back * slope * own_lane).astype(BF)
        for a in range(3):
            lhs1[a * C:(a + 1) * C, plane(q + a - 4)] = grad_pre

    pack_grads(grads_ref, 0, lax.dot_general(
        lhs1[...], wide1[:, 4 * LANES:14 * LANES], NT, preferred_element_type=F32), head_acc[...])

    high = raw_logits[...].astype(BF)
    rest = raw_logits[...] - high.astype(F32)
    middle = rest.astype(BF)
    low = (rest - middle.astype(F32)).astype(BF)
    cell = lax.broadcasted_iota(jnp.int32, (1, 64), 1)
    source = ((cell >> 3) + 4) * 16 + (cell & 7) + 4
    pick = jnp.where(lax.broadcasted_iota(jnp.int32, (LANES, 64), 0) == source, 1.0, 0.0).astype(BF)
    parts = dot32(jnp.concatenate([high, middle, low], axis=0), pick)
    own_logits = (parts[0:64] + parts[64:128]) + parts[128:192]
    for x in range(8):
        logits_ref[:, x * 64:(x + 1) * 64] = own_logits[x * 8:x * 8 + 3]


def compute_block(ids, got, k1, k2, head, scale):
    vmem = pl.BlockSpec(memory_space=pltpu.VMEM)
    v = pltpu.VMEM
    return pl.pallas_call(
        functools.partial(compute_kernel, scale),
        out_shape=(jax.ShapeDtypeStruct((3, 512), F32), jax.ShapeDtypeStruct((2, 32, 16, 128), F32)),
        in_specs=[pl.BlockSpec(memory_space=pltpu.SMEM)] + [vmem] * 4,
        out_specs=(vmem, vmem),
        scratch_shapes=[
            pltpu.SMEM((64,), jnp.int32),
            v((18 * C, 640), BF), v((96, 640), BF),
            v((9 * C, 18 * LANES), BF), v((3 * C, 18 * LANES), F32), v((16, C, LANES), F32),
            v((9 * C, 16 * LANES), BF), v((3 * C, 16 * LANES), F32),
            v((9 * C, 12 * LANES), BF), v((3 * C, 12 * LANES), F32),
            v((3 * C, 12 * LANES), BF), v((3 * C, 10 * LANES), BF),
            v((12, 16, LANES), F32), v((3, 8, LANES), F32), v((16, C), F32),
            v((3 * C, 9 * C), BF), v((3 * C, 9 * C), BF), v((9 * C, 3 * C), BF), v((16, C), F32),
            v((64, LANES), F32),
        ],
        compiler_params=pltpu.CompilerParams(vmem_limit_bytes=60 * 1024 * 1024),
    )(ids, got, k1, k2, head)


MESH = pl.DeviceIdType.MESH
N_Z, N_X = 8, 4
SPLIT = 96


def gather_kernel(features_ref, targets_ref, got_ref, own_ref, wants, send_sem, recv_sem):
    dp, sp = lax.axis_index("dp"), lax.axis_index("space")
    z, x = lax.div(sp, N_X), lax.rem(sp, N_X)

    def at(dz, dx):
        return lax.rem(z + dz + N_Z, N_Z) * N_X + lax.rem(x + dx + N_X, N_X)

    near_by = [(1, 0), (-1, 0), (0, 1), (0, -1), (0, 2)]
    barrier = pltpu.get_barrier_semaphore()
    for dz, dx in near_by:
        pl.semaphore_signal(barrier, inc=1, device_id=(dp, at(dz, dx)), device_id_type=MESH)

    wants[...] = jnp.zeros_like(wants)
    for pair in range(4):
        lanes = slice(pair * 128, (pair + 1) * 128)
        own_ref[pair * C:(pair + 1) * C, :] = features_ref[0, 0, :, lanes]
        wants[pair * 4:pair * 4 + 3, :] = targets_ref[0, 0, :, lanes].astype(F32)
    own_ref[4 * C:4 * C + 16, :] = wants[...].astype(BF)
    got_ref[sp] = own_ref[...]
    pl.semaphore_wait(barrier, len(near_by))

    rows = [pl.ds(0, SPLIT), pl.ds(SPLIT, own_ref.shape[0] - SPLIT)]
    sent = []

    def copy(half, dz, dx, to, number):
        slot = at(dz, dx)
        source = own_ref.at[rows[half]] if (dz, dx) == (0, 0) else got_ref.at[slot, rows[half]]
        return pltpu.make_async_remote_copy(
            src_ref=source, dst_ref=got_ref.at[slot, rows[half]], send_sem=send_sem.at[number],
            recv_sem=recv_sem.at[half, slot], device_id=(dp, at(*to)), device_id_type=MESH)

    def send(half, dz, dx, to):
        one = copy(half, dz, dx, to, len(sent))
        one.start()
        sent.append(one)

    arrived = set()

    def await_block(half, dz, dx):
        if (half, dz, dx) not in arrived and (dz, dx) != (0, 0):
            slot = at(dz, dx)
            pltpu.make_async_remote_copy(
                src_ref=own_ref.at[rows[half]], dst_ref=got_ref.at[slot, rows[half]], send_sem=send_sem.at[0],
                recv_sem=recv_sem.at[half, slot], device_id=(dp, at(0, 1)), device_id_type=MESH).wait_recv()
            arrived.add((half, dz, dx))

    def reach(way, dx):
        return 4 if (way == 1) == (dx in (0, 1)) else 3

    for way in (1, -1):
        send(1, 0, 0, (way, 0))
    for dx in (1, -1, 2):
        send(0, 0, 0, (0, dx))
    for way in (1, -1):
        send(0, 0, 0, (way, 0))
    for dx in (1, -1, 2):
        send(1, 0, 0, (0, dx))

    for k in range(4):
        for dx in (0, 1, -1, 2):
            for way in (1, -1):
                if (k, dx) != (0, 0) and k < reach(way, dx):
                    await_block(0, -way * k, dx)
                    send(0, -way * k, dx, (way, 0))
        for way in (1, -1):
            far = k + 1
            if far <= reach(way, 0):
                await_block(1, -way * far, 0)
                if far < reach(way, 0):
                    send(1, -way * far, 0, (way, 0))
                for dx in (1, -1, 2):
                    send(1, -way * far, 0, (0, dx))

    for half in range(2):
        for dx in (0, 1, -1, 2):
            column = dx if half == 0 else 0
            for way in (1, -1):
                for k in range(reach(way, column) + 1):
                    await_block(half, -way * k, dx)
    for one in sent:
        one.wait_send()


def gather_blocks(features, targets):
    vmem = pl.BlockSpec(memory_space=pltpu.VMEM)
    rows = 4 * C + 16
    return pl.pallas_call(
        gather_kernel,
        out_shape=jax.ShapeDtypeStruct((N_Z * N_X, rows, 128), BF),
        in_specs=[vmem, vmem],
        out_specs=vmem,
        scratch_shapes=[
            pltpu.VMEM((rows, 128), BF), pltpu.VMEM((16, 128), F32),
            pltpu.SemaphoreType.DMA((64,)), pltpu.SemaphoreType.DMA((2, N_Z * N_X))],
        compiler_params=pltpu.CompilerParams(collective_id=1, has_side_effects=True),
    )(features, targets)


def grad_sum_kernel(g_ref, first_ref, second_ref, head_ref, pair_out, pair_in, send_buf, rs_buf, y_buf, done,
                    pair_send, pair_sem, rs_send, rs_sem, y_send, y_sem, ag_send, ag_sem, last_send, last_sem):
    dp, sp = lax.axis_index("dp"), lax.axis_index("space")
    core, y = lax.rem(dp, 2), lax.div(dp, 2)
    n_y, n_sp = y_buf.shape[0], rs_buf.shape[0]
    partner = (dp + 1 - 2 * core, sp)

    def along(r):
        return lax.rem(sp + r, n_sp)

    def line(r):
        return (lax.rem(y + r, n_y) * 2 + core, sp)

    barrier = pltpu.get_barrier_semaphore()
    pl.semaphore_signal(barrier, inc=1, device_id=partner, device_id_type=MESH)
    for r in range(1, n_sp):
        pl.semaphore_signal(barrier, inc=1, device_id=(dp, along(r)), device_id_type=MESH)
    for r in range(1, n_y):
        pl.semaphore_signal(barrier, inc=1, device_id=line(r), device_id_type=MESH)
    pair_out[...] = g_ref[1 - core].astype(BF)
    pl.semaphore_wait(barrier, n_sp + n_y - 1)

    def remote(source, target, send, receive, device):
        return pltpu.make_async_remote_copy(
            src_ref=source, dst_ref=target, send_sem=send, recv_sem=receive, device_id=device, device_id_type=MESH)

    pair_copy = remote(pair_out, pair_in, pair_send, pair_sem, partner)
    pair_copy.start()
    pair_copy.wait_recv()
    send_buf[...] = (g_ref[core] + pair_in[...].astype(F32)).astype(BF)

    def rs_copy(r):
        return remote(send_buf.at[along(r)], rs_buf.at[r], rs_send.at[r], rs_sem.at[r], (dp, along(r)))

    def y_copy(r):
        return remote(y_buf.at[0], y_buf.at[r], y_send.at[r], y_sem.at[r], line(r))

    def ag_copy(r):
        return remote(done.at[core, sp], done.at[core, sp], ag_send.at[r], ag_sem.at[r], (dp, along(r)))

    def last_copy(r):
        slot = lax.rem(sp - r + n_sp, n_sp)
        return remote(done.at[core, slot], done.at[core, slot], last_send.at[r], last_sem.at[r], partner)

    for r in range(1, n_sp):
        rs_copy(r).start()
    total = g_ref[core, sp] + pair_in[sp].astype(F32)
    for r in range(1, n_sp):
        rs_copy(r).wait_recv()
        total = total + rs_buf[r].astype(F32)
    y_buf[0] = total.astype(BF)
    for r in range(1, n_y):
        y_copy(r).start()
    for r in range(1, n_y):
        y_copy(r).wait_recv()
    total = jnp.zeros(total.shape, F32)
    for d in range(n_y):
        total = total + y_buf[lax.rem(y - d + n_y, n_y)].astype(F32)
    done[core, sp] = total.astype(BF)
    for r in range(1, n_sp):
        ag_copy(r).start()
    last_copy(0).start()
    for r in range(1, n_sp):
        slot = lax.rem(sp - r + n_sp, n_sp)
        remote(done.at[core, slot], done.at[core, slot], ag_send.at[r], ag_sem.at[r], (dp, along(r))).wait_recv()
        last_copy(r).start()
    for r in range(n_sp):
        slot = lax.rem(sp - r + n_sp, n_sp)
        remote(done.at[1 - core, slot], done.at[1 - core, slot], last_send.at[r], last_sem.at[r], partner).wait_recv()

    for part, out in enumerate((first_ref, second_ref)):
        for group in range(9):
            a, rows = group // 3, slice(group % 3 * 16, group % 3 * 16 + 16)
            tail = done[part, 27 + group // 2].astype(F32)
            out[a * 9 + 8, rows, :] = tail[:, 64 * (group % 2):64 * (group % 2) + C]
            wide = jnp.concatenate([done[part, group * 3 + col].astype(F32) for col in range(3)], axis=1)
            for bc in range(8):
                out[a * 9 + bc, rows, :] = wide[:, bc * C:(bc + 1) * C]
    head_ref[...] = done[0, 31].astype(F32)[0:3, 64:64 + C]

    pair_copy.wait_send()
    for r in range(1, n_sp):
        rs_copy(r).wait_send()
        ag_copy(r).wait_send()
    for r in range(1, n_y):
        y_copy(r).wait_send()
    for r in range(n_sp):
        last_copy(r).wait_send()


def grad_sum(grads):
    n_y, n_sp = lax.axis_size("dp") // 2, lax.axis_size("space")
    vmem = pl.BlockSpec(memory_space=pltpu.VMEM)
    dma = pltpu.SemaphoreType.DMA
    half = pltpu.VMEM((n_sp, 16, 128), BF)
    kernel = jax.ShapeDtypeStruct((27, C, C), F32)
    return pl.pallas_call(
        grad_sum_kernel,
        out_shape=(kernel, kernel, jax.ShapeDtypeStruct((3, C), F32)),
        in_specs=[vmem],
        out_specs=(vmem, vmem, vmem),
        scratch_shapes=[
            half, half, half, half, pltpu.VMEM((n_y, 16, 128), BF), pltpu.VMEM((2, n_sp, 16, 128), BF),
            dma, dma, dma((n_sp,)), dma((n_sp,)), dma((n_y,)), dma((n_y,)), dma((n_sp,)), dma((n_sp,)),
            dma((n_sp,)), dma((n_sp,)),
        ],
        compiler_params=pltpu.CompilerParams(collective_id=0, has_side_effects=True),
    )(grads)


def on_device(features, device_block, conv_first, conv_second, head_weight, targets):
    n_dp, n_sp = lax.axis_size("dp"), lax.axis_size("space")
    scale = (n_dp * n_sp * 3 * 512) ** (-0.5)
    got = gather_blocks(features, targets)
    logits, grads = compute_block(
        device_block, got, conv_first.transpose(1, 0, 2), conv_second.transpose(1, 0, 2), head_weight, scale)
    first, second, head = grad_sum(grads)
    return (logits[None, None], first.transpose(1, 0, 2), second.transpose(1, 0, 2), head)


def solution(mesh):
    in_specs = (
        P("dp", "space", None, None),
        P("dp", None),
        P(),
        P(),
        P(),
        P("dp", "space", None, None),
    )
    out_specs = (P("dp", "space", None, None), P(), P(), P())
    return jax.shard_map(
        on_device, mesh=mesh, in_specs=in_specs, out_specs=out_specs, check_vma=False
    )
```

```python
import functools
import jax
import jax.numpy as jnp
from jax import lax
from jax.experimental import pallas as pl
from jax.experimental.pallas import tpu as pltpu
from jax.sharding import PartitionSpec as P

BF = jnp.bfloat16
F32 = jnp.float32
C = 48
LANES = 256
NT = (((1,), (1,)), ((), ()))
TN = (((0,), (0,)), ((), ()))


def dot32(a, b):
    return jnp.dot(a, b, preferred_element_type=F32)


def elu_pair(values):
    negative = jnp.exp(jnp.minimum(values, 0.0))
    return (jnp.where(values > 0, values, negative - 1.0), jnp.where(values > 0, 1.0, negative))


def plane(index):
    start = index * LANES
    return pl.ds(start if isinstance(index, int) else pl.multiple_of(start, LANES), LANES)


def pack_grads(grads_ref, part, grads, head):
    for group in range(9):
        rows = grads[group * 16:(group + 1) * 16]
        for col in range(3):
            grads_ref[part, group * 3 + col] = rows[:, col * 128:(col + 1) * 128]
        grads_ref[part, 27 + group // 2, :, 64 * (group % 2):64 * (group % 2) + C] = rows[:, 384:9 * C]
    grads_ref[part, 31, :, 64:64 + C] = head


def compute_kernel(scale, ids_ref, got_ref, k1_ref, k2_ref, head_in_ref,
                   logits_ref, grads_ref,
                   table, near, near_t, faces, wide1, out1, pre1, wide2, out2, wide_b, out_b, lhs2, lhs1, want,
                   mask_ref, mask2, hid2, slope2, back2, w1_ref, w2_ref, wb_ref, head_ref, raw_logits):
    me = lax.axis_index("space")

    for t in range(27):
        a, bc = t // 9, t % 9
        w1_ref[a * C:(a + 1) * C, bc * C:(bc + 1) * C] = k1_ref[t]
        w2_ref[a * C:(a + 1) * C, bc * C:(bc + 1) * C] = k2_ref[t]
        wb_ref[bc * C:(bc + 1) * C, a * C:(a + 1) * C] = k2_ref[t]
    head_ref[...] = jnp.zeros_like(head_ref)
    head_ref[0:3, :] = head_in_ref[...].astype(F32)
    head = head_ref[...].astype(BF)
    head_t = head_ref[...].T.astype(BF)

    @pl.loop(0, 64)
    def _(i):
        table[i] = -1

    @pl.loop(0, 32)
    def _(j):
        table[ids_ref[0, j]] = j

    own = ids_ref[0, me]
    ox, oy, oz = own // 16, own // 4 % 4, own % 4
    slots, present = [], []
    for t in range(27):
        x, y, z = ox + t // 9 - 1, oy + t // 3 % 3 - 1, oz + t % 3 - 1
        inside = (x >= 0) & (x < 4) & (y >= 0) & (y < 4) & (z >= 0) & (z < 4)
        found = table[jnp.where(inside, (x * 4 + y) * 4 + z, own)]
        ok = inside & (found >= 0)
        slots.append(jnp.where(ok, found, me))
        present.append(jnp.where(ok, 1.0, 0.0).astype(F32))

    low_half = lax.broadcasted_iota(jnp.int32, (C, 128), 1) < 64

    def tiles_of(bx, by, row, rows):
        return [
            (got_ref[slots[t], row:row + rows, :].astype(F32) * present[t]).astype(BF)
            for t in (bx * 9 + by * 3 + bz for bz in range(3))
        ]

    def face_pair(tiles, half):
        keep = low_half[:tiles[0].shape[0]]
        flip = lambda v: pltpu.roll(v, 64, 1)
        first = tiles[0] if half == 0 else flip(tiles[0])
        second = tiles[1] if half == 1 else flip(tiles[1])
        third = tiles[2] if half == 0 else flip(tiles[2])
        return jnp.where(keep, first, second), jnp.where(keep, third, jnp.zeros_like(third))

    for bx in range(3):
        for by in range(3):
            for pair in range(4):
                spots = [(half, bx * 8 + pair * 2 + half - 3) for half in range(2)]
                spots = [(half, at) for half, at in spots if 0 <= at < 18]
                if not spots:
                    continue
                tiles = tiles_of(bx, by, pair * C, C)
                for half, at in spots:
                    for k, value in enumerate(face_pair(tiles, half)):
                        near[by, at * C:(at + 1) * C, k * 128:(k + 1) * 128] = value
            tiles = tiles_of(bx, by, 4 * C, 16)
            for half in range(2):
                at = bx * 2 + half
                for k, value in enumerate(face_pair(tiles, half)):
                    near_t[by, at * 16:(at + 1) * 16, k * 128:(k + 1) * 128] = value

    column = lax.broadcasted_iota(jnp.int32, (1, 3 * 128), 1)
    z = (column & 15) + (column >> 7) + 3
    source = (z >> 3) * 64 + ((column >> 4) & 7) * 8 + (z & 7)
    pick_z = jnp.where(lax.broadcasted_iota(jnp.int32, (LANES, 3 * 128), 0) == source, 1.0, 0.0).astype(BF)
    want[...] = jnp.zeros_like(want)
    wanted = [dot32(near_t[by], pick_z[:, 128:256]) for by in range(3)]
    for by in range(3):
        faces[by] = dot32(near[by], pick_z).astype(BF)

    def window(plane_24, start):
        return pltpu.roll(plane_24, 384 - start, 1)[:, :LANES]

    @pl.loop(0, 18)
    def _(at):
        rows = pl.ds(pl.multiple_of(at * C, 16), C)
        for c in range(3):
            tall = jnp.concatenate([faces[by, rows, c * 128:(c + 1) * 128] for by in range(3)], axis=1)
            for b in range(3):
                wide1[(b * 3 + c) * C:(b * 3 + c + 1) * C, plane(at)] = window(tall, 48 + 16 * b)

    for at in range(6):
        tall = window(jnp.concatenate([one[at * 16:(at + 1) * 16] for one in wanted], axis=1), 64)
        for pair in range(4):
            xo = (at // 2 - 1) * 8 + pair * 2 + at % 2 + 4
            if 2 <= xo < 14:
                want[0:3, plane(xo - 2)] = tall[pair * 4:pair * 4 + 3]

    lane = lax.broadcasted_iota(jnp.int32, (1, LANES), 1)
    y, z = lane >> 4, lane & 15
    region = ((y + 4) >> 3) * 3 + ((z + 4) >> 3)
    inner = jnp.where((y >= 2) & (y < 14) & (z >= 2) & (z < 14), 1.0, 0.0)
    own_lane = jnp.where((y >= 4) & (y < 12) & (z >= 4) & (z < 12), 1.0, 0.0)
    for bx in range(3):
        row = jnp.zeros((1, LANES), F32)
        for j in range(9):
            row = jnp.where(region == j, present[bx * 9 + j], row)
        mask_ref[bx, 0:1, :] = row
        for xo in range(2, 14):
            if (xo + 4) // 8 == bx:
                mask2[0:1, plane(xo - 2)] = row * inner
                mask2[1:2, plane(xo - 2)] = own_lane if bx == 1 else jnp.zeros_like(own_lane)

    out1[...] = dot32(w1_ref[...], wide1[...])

    def first_plane(xo, carry):
        pre = out1[0:C, plane(xo)] + out1[C:2 * C, plane(xo + 1)] + out1[2 * C:3 * C, plane(xo + 2)]
        pre1[xo] = pre
        act, _slope = elu_pair(pre)
        hid = (act * mask_ref[lax.div(xo + 4, 8), 0:1, :]).astype(BF)
        for bc in range(9):
            shift = -(32 * (bc // 3 - 1) + 2 * (bc % 3 - 1)) % LANES
            wide2[bc * C:(bc + 1) * C, plane(xo)] = pltpu.roll(hid, shift, 1) if shift else hid
        return carry

    lax.fori_loop(0, 16, first_plane, 0, unroll=2)

    out2[...] = dot32(w2_ref[...], wide2[...])
    lhs2[...] = jnp.zeros_like(lhs2)
    lhs1[...] = jnp.zeros_like(lhs1)

    def second_plane(i, carry):
        pre = out2[0:C, plane(i)] + out2[C:2 * C, plane(i + 2)] + out2[2 * C:3 * C, plane(i + 4)]
        act, slope = elu_pair(pre)
        mask = mask2[0:1, plane(i)]
        hid2[:, plane(i)] = (act * mask).astype(BF)
        slope2[:, plane(i)] = slope * mask
        return carry

    lax.fori_loop(0, 12, second_plane, 0, unroll=2)
    logits = dot32(head, hid2[...])
    for x in range(8):
        raw_logits[x * 8:(x + 1) * 8, :] = logits[0:8, (x + 2) * LANES:(x + 3) * LANES]
    grad_logit = (jax.nn.sigmoid(logits) - want[...]) * mask2[0:1, :] * scale
    own_logit = (grad_logit * mask2[1:2, :]).astype(BF)
    back2[...] = dot32(head_t, grad_logit.astype(BF))
    head_grad = lax.dot_general(own_logit, hid2[...], NT, preferred_element_type=F32)

    def grad_plane(i, is_own):
        grad_pre = (back2[:, plane(i)] * slope2[:, plane(i)]).astype(BF)
        for bc in range(9):
            shift = (32 * (bc // 3 - 1) + 2 * (bc % 3 - 1)) % LANES
            wide_b[bc * C:(bc + 1) * C, plane(i)] = pltpu.roll(grad_pre, shift, 1) if shift else grad_pre
        if is_own:
            own_pre = (grad_pre.astype(F32) * own_lane).astype(BF)
            for a in range(3):
                lhs2[a * C:(a + 1) * C, plane(i + 2 * a - 2)] = own_pre

    def own_plane(i, carry):
        grad_plane(i + 2, True)
        return carry

    lax.fori_loop(0, 8, own_plane, 0, unroll=2)
    for i in (0, 1, 10, 11):
        grad_plane(i, False)

    grads_ref[:, 27:32] = jnp.zeros((2, 5, 16, 128), F32)
    pack_grads(grads_ref, 1, lax.dot_general(
        lhs2[...], wide2[:, 2 * LANES:14 * LANES], NT, preferred_element_type=F32), jnp.zeros((16, C), F32))
    out_b[...] = lax.dot_general(wb_ref[...], wide_b[...], TN, preferred_element_type=F32)

    @pl.loop(4, 12)
    def _(q):
        back = out_b[0:C, plane(q)] + out_b[C:2 * C, plane(q - 2)] + out_b[2 * C:3 * C, plane(q - 4)]
        _act, slope = elu_pair(pre1[q])
        grad_pre = (back * slope * own_lane).astype(BF)
        for a in range(3):
            lhs1[a * C:(a + 1) * C, plane(q + a - 4)] = grad_pre

    pack_grads(grads_ref, 0, lax.dot_general(
        lhs1[...], wide1[:, 4 * LANES:14 * LANES], NT, preferred_element_type=F32), head_grad)

    high = raw_logits[...].astype(BF)
    rest = raw_logits[...] - high.astype(F32)
    middle = rest.astype(BF)
    low = (rest - middle.astype(F32)).astype(BF)
    cell = lax.broadcasted_iota(jnp.int32, (1, 64), 1)
    source = ((cell >> 3) + 4) * 16 + (cell & 7) + 4
    pick = jnp.where(lax.broadcasted_iota(jnp.int32, (LANES, 64), 0) == source, 1.0, 0.0).astype(BF)
    parts = dot32(jnp.concatenate([high, middle, low], axis=0), pick)
    own_logits = (parts[0:64] + parts[64:128]) + parts[128:192]
    for x in range(8):
        logits_ref[:, x * 64:(x + 1) * 64] = own_logits[x * 8:x * 8 + 3]


def compute_block(ids, got, k1, k2, head, scale):
    vmem = pl.BlockSpec(memory_space=pltpu.VMEM)
    v = pltpu.VMEM
    return pl.pallas_call(
        functools.partial(compute_kernel, scale),
        out_shape=(jax.ShapeDtypeStruct((3, 512), F32), jax.ShapeDtypeStruct((2, 32, 16, 128), F32)),
        in_specs=[pl.BlockSpec(memory_space=pltpu.SMEM)] + [vmem] * 4,
        out_specs=(vmem, vmem),
        scratch_shapes=[
            pltpu.SMEM((64,), jnp.int32),
            v((3, 18 * C, LANES), BF), v((3, 96, LANES), BF), v((3, 18 * C, 3 * 128), BF),
            v((9 * C, 18 * LANES), BF), v((3 * C, 18 * LANES), F32), v((16, C, LANES), F32),
            v((9 * C, 16 * LANES), BF), v((3 * C, 16 * LANES), F32),
            v((9 * C, 12 * LANES), BF), v((3 * C, 12 * LANES), F32),
            v((3 * C, 12 * LANES), BF), v((3 * C, 10 * LANES), BF),
            v((16, 12 * LANES), F32), v((3, 8, LANES), F32), v((8, 12 * LANES), F32),
            v((C, 12 * LANES), BF), v((C, 12 * LANES), F32), v((C, 12 * LANES), F32),
            v((3 * C, 9 * C), BF), v((3 * C, 9 * C), BF), v((9 * C, 3 * C), BF), v((16, C), F32),
            v((64, LANES), F32),
        ],
        compiler_params=pltpu.CompilerParams(vmem_limit_bytes=60 * 1024 * 1024),
    )(ids, got, k1, k2, head)


MESH = pl.DeviceIdType.MESH
N_Z, N_X = 8, 4
SPLIT = 48
Z_STEPS = (1, -1, 2, -2, 3, -3, 4)
X_STEPS = (1, -1, 2)


def gather_kernel(features_ref, targets_ref, got_ref, own_ref, wants, send_sem, recv_sem):
    dp, sp = lax.axis_index("dp"), lax.axis_index("space")
    z, x = lax.div(sp, N_X), lax.rem(sp, N_X)

    def at(dz, dx):
        return lax.rem(z + dz + N_Z, N_Z) * N_X + lax.rem(x + dx + N_X, N_X)

    near_by = [(dz, 0) for dz in Z_STEPS] + [(0, dx) for dx in X_STEPS]
    barrier = pltpu.get_barrier_semaphore()
    for dz, dx in near_by:
        pl.semaphore_signal(barrier, inc=1, device_id=(dp, at(dz, dx)), device_id_type=MESH)

    wants[...] = jnp.zeros_like(wants)
    for pair in range(4):
        lanes = slice(pair * 128, (pair + 1) * 128)
        own_ref[pair * C:(pair + 1) * C, :] = features_ref[0, 0, :, lanes]
        wants[pair * 4:pair * 4 + 3, :] = targets_ref[0, 0, :, lanes].astype(F32)
    own_ref[4 * C:4 * C + 16, :] = wants[...].astype(BF)
    got_ref[sp] = own_ref[...]
    pl.semaphore_wait(barrier, len(near_by))

    rows = [pl.ds(0, SPLIT), pl.ds(SPLIT, own_ref.shape[0] - SPLIT)]
    sent = []

    def copy(half, dz, dx, to, number):
        slot = at(dz, dx)
        source = own_ref.at[rows[half]] if (dz, dx) == (0, 0) else got_ref.at[slot, rows[half]]
        return pltpu.make_async_remote_copy(
            src_ref=source, dst_ref=got_ref.at[slot, rows[half]], send_sem=send_sem.at[number],
            recv_sem=recv_sem.at[half, slot], device_id=(dp, at(*to)), device_id_type=MESH)

    def send(half, dz, dx, to):
        one = copy(half, dz, dx, to, len(sent))
        one.start()
        sent.append(one)

    def await_block(half, dz, dx):
        slot = at(dz, dx)
        pltpu.make_async_remote_copy(
            src_ref=own_ref.at[rows[half]], dst_ref=got_ref.at[slot, rows[half]], send_sem=send_sem.at[0],
            recv_sem=recv_sem.at[half, slot], device_id=(dp, at(0, 1)), device_id_type=MESH).wait_recv()

    for dx in X_STEPS:
        send(0, 0, 0, (0, dx))
    for dz in Z_STEPS:
        send(1, 0, 0, (dz, 0))
    for dx in X_STEPS:
        send(1, 0, 0, (0, dx))
    for dz in Z_STEPS:
        send(0, 0, 0, (dz, 0))

    def pass_x(dx):
        await_block(0, 0, dx)
        for dz in Z_STEPS:
            send(0, 0, dx, (dz, 0))

    def pass_z(dz):
        await_block(1, dz, 0)
        for dx in X_STEPS:
            send(1, dz, 0, (0, dx))

    for dz in (1, -1):
        pass_z(dz)
    for dx in X_STEPS:
        pass_x(dx)
    for dz in (2, -2, 3, -3, 4):
        pass_z(dz)
    for dz in Z_STEPS:
        for dx in (0, *X_STEPS):
            await_block(0, dz, dx)
    for dz in (0, *Z_STEPS):
        for dx in X_STEPS:
            await_block(1, dz, dx)
    for one in sent:
        one.wait_send()


def gather_blocks(features, targets):
    vmem = pl.BlockSpec(memory_space=pltpu.VMEM)
    rows = 4 * C + 16
    return pl.pallas_call(
        gather_kernel,
        out_shape=jax.ShapeDtypeStruct((N_Z * N_X, rows, 128), BF),
        in_specs=[vmem, vmem],
        out_specs=vmem,
        scratch_shapes=[
            pltpu.VMEM((rows, 128), BF), pltpu.VMEM((16, 128), F32),
            pltpu.SemaphoreType.DMA((64,)), pltpu.SemaphoreType.DMA((2, N_Z * N_X))],
        compiler_params=pltpu.CompilerParams(collective_id=1, has_side_effects=True),
    )(features, targets)


def grad_sum_kernel(g_ref, first_ref, second_ref, head_ref, pair_out, pair_in, send_buf, rs_buf, y_buf, done,
                    pair_send, pair_sem, rs_send, rs_sem, y_send, y_sem, ag_send, ag_sem, last_send, last_sem):
    dp, sp = lax.axis_index("dp"), lax.axis_index("space")
    core, y = lax.rem(dp, 2), lax.div(dp, 2)
    n_y, n_sp = y_buf.shape[0], rs_buf.shape[0]
    partner = (dp + 1 - 2 * core, sp)

    def along(r):
        return lax.rem(sp + r, n_sp)

    def line(r):
        return (lax.rem(y + r, n_y) * 2 + core, sp)

    barrier = pltpu.get_barrier_semaphore()
    pl.semaphore_signal(barrier, inc=1, device_id=partner, device_id_type=MESH)
    for r in range(1, n_sp):
        pl.semaphore_signal(barrier, inc=1, device_id=(dp, along(r)), device_id_type=MESH)
    for r in range(1, n_y):
        pl.semaphore_signal(barrier, inc=1, device_id=line(r), device_id_type=MESH)
    pair_out[...] = g_ref[1 - core].astype(BF)
    pl.semaphore_wait(barrier, n_sp + n_y - 1)

    def remote(source, target, send, receive, device):
        return pltpu.make_async_remote_copy(
            src_ref=source, dst_ref=target, send_sem=send, recv_sem=receive, device_id=device, device_id_type=MESH)

    pair_copy = remote(pair_out, pair_in, pair_send, pair_sem, partner)
    pair_copy.start()
    pair_copy.wait_recv()
    send_buf[...] = (g_ref[core] + pair_in[...].astype(F32)).astype(BF)

    def rs_copy(r):
        return remote(send_buf.at[along(r)], rs_buf.at[r], rs_send.at[r], rs_sem.at[r], (dp, along(r)))

    def y_copy(r):
        return remote(y_buf.at[0], y_buf.at[r], y_send.at[r], y_sem.at[r], line(r))

    def ag_copy(r):
        return remote(done.at[core, sp], done.at[core, sp], ag_send.at[r], ag_sem.at[r], (dp, along(r)))

    def last_copy(r):
        slot = lax.rem(sp - r + n_sp, n_sp)
        return remote(done.at[core, slot], done.at[core, slot], last_send.at[r], last_sem.at[r], partner)

    for r in range(1, n_sp):
        rs_copy(r).start()
    total = g_ref[core, sp] + pair_in[sp].astype(F32)
    for r in range(1, n_sp):
        rs_copy(r).wait_recv()
        total = total + rs_buf[r].astype(F32)
    y_buf[0] = total.astype(BF)
    for r in range(1, n_y):
        y_copy(r).start()
    for r in range(1, n_y):
        y_copy(r).wait_recv()
    total = jnp.zeros(total.shape, F32)
    for d in range(n_y):
        total = total + y_buf[lax.rem(y - d + n_y, n_y)].astype(F32)
    done[core, sp] = total.astype(BF)
    for r in range(1, n_sp):
        ag_copy(r).start()
    last_copy(0).start()
    for r in range(1, n_sp):
        slot = lax.rem(sp - r + n_sp, n_sp)
        remote(done.at[core, slot], done.at[core, slot], ag_send.at[r], ag_sem.at[r], (dp, along(r))).wait_recv()
        last_copy(r).start()
    for r in range(n_sp):
        slot = lax.rem(sp - r + n_sp, n_sp)
        remote(done.at[1 - core, slot], done.at[1 - core, slot], last_send.at[r], last_sem.at[r], partner).wait_recv()

    for part, out in enumerate((first_ref, second_ref)):
        for group in range(9):
            a, rows = group // 3, slice(group % 3 * 16, group % 3 * 16 + 16)
            tail = done[part, 27 + group // 2].astype(F32)
            out[a * 9 + 8, rows, :] = tail[:, 64 * (group % 2):64 * (group % 2) + C]
            wide = jnp.concatenate([done[part, group * 3 + col].astype(F32) for col in range(3)], axis=1)
            for bc in range(8):
                out[a * 9 + bc, rows, :] = wide[:, bc * C:(bc + 1) * C]
    head_ref[...] = done[0, 31].astype(F32)[0:3, 64:64 + C]

    pair_copy.wait_send()
    for r in range(1, n_sp):
        rs_copy(r).wait_send()
        ag_copy(r).wait_send()
    for r in range(1, n_y):
        y_copy(r).wait_send()
    for r in range(n_sp):
        last_copy(r).wait_send()


def grad_sum(grads):
    n_y, n_sp = lax.axis_size("dp") // 2, lax.axis_size("space")
    vmem = pl.BlockSpec(memory_space=pltpu.VMEM)
    dma = pltpu.SemaphoreType.DMA
    half = pltpu.VMEM((n_sp, 16, 128), BF)
    kernel = jax.ShapeDtypeStruct((27, C, C), F32)
    return pl.pallas_call(
        grad_sum_kernel,
        out_shape=(kernel, kernel, jax.ShapeDtypeStruct((3, C), F32)),
        in_specs=[vmem],
        out_specs=(vmem, vmem, vmem),
        scratch_shapes=[
            half, half, half, half, pltpu.VMEM((n_y, 16, 128), BF), pltpu.VMEM((2, n_sp, 16, 128), BF),
            dma, dma, dma((n_sp,)), dma((n_sp,)), dma((n_y,)), dma((n_y,)), dma((n_sp,)), dma((n_sp,)),
            dma((n_sp,)), dma((n_sp,)),
        ],
        compiler_params=pltpu.CompilerParams(collective_id=0, has_side_effects=True),
    )(grads)


def on_device(features, device_block, conv_first, conv_second, head_weight, targets):
    n_dp, n_sp = lax.axis_size("dp"), lax.axis_size("space")
    scale = (n_dp * n_sp * 3 * 512) ** (-0.5)
    got = gather_blocks(features, targets)
    logits, grads = compute_block(
        device_block, got, conv_first.transpose(1, 0, 2), conv_second.transpose(1, 0, 2), head_weight, scale)
    first, second, head = grad_sum(grads)
    return (logits[None, None], first.transpose(1, 0, 2), second.transpose(1, 0, 2), head)


def solution(mesh):
    in_specs = (
        P("dp", "space", None, None),
        P("dp", None),
        P(),
        P(),
        P(),
        P("dp", "space", None, None),
    )
    out_specs = (P("dp", "space", None, None), P(), P(), P())
    return jax.shard_map(
        on_device, mesh=mesh, in_specs=in_specs, out_specs=out_specs, check_vma=False
    )
```

```python
import functools
from types import SimpleNamespace

import jax
import jax.numpy as jnp
from jax import lax
from jax.experimental import pallas as pl
from jax.experimental.pallas import tpu as pltpu
from jax.sharding import PartitionSpec as P

BF = jnp.bfloat16
F32 = jnp.float32
C = 48
LANES = 256
NT = (((1,), (1,)), ((), ()))
TN = (((0,), (0,)), ((), ()))


def dot32(a, b):
    return jnp.dot(a, b, preferred_element_type=F32)


def elu_pair(values):
    negative = jnp.exp(jnp.minimum(values, 0.0))
    return (jnp.where(values > 0, values, negative - 1.0), jnp.where(values > 0, 1.0, negative))


def plane(index):
    start = index * LANES
    return pl.ds(start if isinstance(index, int) else pl.multiple_of(start, LANES), LANES)


def pack_grads(grads_ref, part, grads, head):
    for group in range(9):
        rows = grads[group * 16:(group + 1) * 16]
        for col in range(3):
            grads_ref[part, group * 3 + col] = rows[:, col * 128:(col + 1) * 128]
        grads_ref[part, 27 + group // 2, :, 64 * (group % 2):64 * (group % 2) + C] = rows[:, 384:9 * C]
    grads_ref[part, 31, :, 64:64 + C] = head


MESH = pl.DeviceIdType.MESH
N_Z, N_X, N_Y = 8, 4, 8
SPLIT = 48
Z_STEPS = (1, -1, 2, -2, 3, -3, 4)
X_STEPS = (1, -1, 2)


def gather_stage(features_ref, targets_ref, got_ref, own_ref, wants, send_sem, recv_sem, meanwhile):
    dp, sp = lax.axis_index("dp"), lax.axis_index("space")
    z, x = lax.div(sp, N_X), lax.rem(sp, N_X)

    def at(dz, dx):
        return lax.rem(z + dz + N_Z, N_Z) * N_X + lax.rem(x + dx + N_X, N_X)

    near_by = [(dz, 0) for dz in Z_STEPS] + [(0, dx) for dx in X_STEPS]
    barrier = pltpu.get_barrier_semaphore()
    for dz, dx in near_by:
        pl.semaphore_signal(barrier, inc=1, device_id=(dp, at(dz, dx)), device_id_type=MESH)
    others = [(dp + 1 - 2 * lax.rem(dp, 2), sp)] + [(lax.rem(dp + 2 * r, N_Y * 2), sp) for r in range(1, N_Y)]
    for other in others:
        pl.semaphore_signal(barrier, inc=1, device_id=other, device_id_type=MESH)

    wants[...] = jnp.zeros_like(wants)
    for pair in range(4):
        lanes = slice(pair * 128, (pair + 1) * 128)
        own_ref[pair * C:(pair + 1) * C, :] = features_ref[0, 0, :, lanes]
        wants[pair * 4:pair * 4 + 3, :] = targets_ref[0, 0, :, lanes].astype(F32)
    own_ref[4 * C:4 * C + 16, :] = wants[...].astype(BF)
    got_ref[sp] = own_ref[...]
    pl.semaphore_wait(barrier, len(near_by) + len(others))

    rows = [pl.ds(0, SPLIT), pl.ds(SPLIT, own_ref.shape[0] - SPLIT)]
    sent = []

    def copy(half, dz, dx, to, number):
        slot = at(dz, dx)
        source = own_ref.at[rows[half]] if (dz, dx) == (0, 0) else got_ref.at[slot, rows[half]]
        return pltpu.make_async_remote_copy(
            src_ref=source, dst_ref=got_ref.at[slot, rows[half]], send_sem=send_sem.at[number],
            recv_sem=recv_sem.at[half, slot], device_id=(dp, at(*to)), device_id_type=MESH)

    def send(half, dz, dx, to):
        one = copy(half, dz, dx, to, len(sent))
        one.start()
        sent.append(one)

    def await_block(half, dz, dx):
        slot = at(dz, dx)
        pltpu.make_async_remote_copy(
            src_ref=own_ref.at[rows[half]], dst_ref=got_ref.at[slot, rows[half]], send_sem=send_sem.at[0],
            recv_sem=recv_sem.at[half, slot], device_id=(dp, at(0, 1)), device_id_type=MESH).wait_recv()

    for dx in X_STEPS:
        send(0, 0, 0, (0, dx))
    for dz in Z_STEPS:
        send(1, 0, 0, (dz, 0))
    for dx in X_STEPS:
        send(1, 0, 0, (0, dx))
    for dz in Z_STEPS:
        send(0, 0, 0, (dz, 0))
    meanwhile()

    def pass_x(dx):
        await_block(0, 0, dx)
        for dz in Z_STEPS:
            send(0, 0, dx, (dz, 0))

    def pass_z(dz):
        await_block(1, dz, 0)
        for dx in X_STEPS:
            send(1, dz, 0, (0, dx))

    for dz in (1, -1):
        pass_z(dz)
    for dx in X_STEPS:
        pass_x(dx)
    for dz in (2, -2, 3, -3, 4):
        pass_z(dz)
    for dz in Z_STEPS:
        for dx in (0, *X_STEPS):
            await_block(0, dz, dx)
    for dz in (0, *Z_STEPS):
        for dx in X_STEPS:
            await_block(1, dz, dx)
    return sent


def prepare(s, ids_ref, k1_ref, k2_ref, head_in_ref):
    for t in range(27):
        a, bc = t // 9, t % 9
        s.w1_ref[a * C:(a + 1) * C, bc * C:(bc + 1) * C] = k1_ref[t]
        s.w2_ref[a * C:(a + 1) * C, bc * C:(bc + 1) * C] = k2_ref[t]
        s.wb_ref[bc * C:(bc + 1) * C, a * C:(a + 1) * C] = k2_ref[t]
    s.head_ref[...] = jnp.zeros_like(s.head_ref)
    s.head_ref[0:3, :] = head_in_ref[...].astype(F32)

    column = lax.broadcasted_iota(jnp.int32, (1, 3 * 128), 1)
    z = (column & 15) + (column >> 7) + 3
    source = (z >> 3) * 64 + ((column >> 4) & 7) * 8 + (z & 7)
    s.pick_ref[...] = jnp.where(lax.broadcasted_iota(jnp.int32, (LANES, 3 * 128), 0) == source, 1.0, 0.0).astype(BF)
    for ref in (s.want, s.lhs2, s.lhs1):
        ref[...] = jnp.zeros_like(ref)
    s.grads_ref[:, 27:32] = jnp.zeros((2, 5, 16, 128), F32)

    own = ids_ref[0, lax.axis_index("space")]
    ox, oy, oz = own // 16, own // 4 % 4, own % 4

    @pl.loop(0, 27)
    def _(t):
        x, y, z = ox + t // 9 - 1, oy + t // 3 % 3 - 1, oz + t % 3 - 1
        inside = (x >= 0) & (x < 4) & (y >= 0) & (y < 4) & (z >= 0) & (z < 4)
        wanted = jnp.where(inside, (x * 4 + y) * 4 + z, -1)
        found = jnp.int32(-1)
        for j in range(32):
            found = jnp.where(ids_ref[0, j] == wanted, j, found)
        s.table[t] = found


def compute(s, scale):
    slots = [jnp.maximum(s.table[t], 0) for t in range(27)]
    present = [jnp.where(s.table[t] >= 0, 1.0, 0.0).astype(F32) for t in range(27)]
    head = s.head_ref[...].astype(BF)
    head_t = s.head_ref[...].T.astype(BF)

    low_half = lax.broadcasted_iota(jnp.int32, (C, 128), 1) < 64

    def tiles_of(bx, by, row, rows):
        return [
            (s.got[slots[t], row:row + rows, :].astype(F32) * present[t]).astype(BF)
            for t in (bx * 9 + by * 3 + bz for bz in range(3))
        ]

    def face_pair(tiles, half):
        keep = low_half[:tiles[0].shape[0]]
        flip = lambda v: pltpu.roll(v, 64, 1)
        first = tiles[0] if half == 0 else flip(tiles[0])
        second = tiles[1] if half == 1 else flip(tiles[1])
        third = tiles[2] if half == 0 else flip(tiles[2])
        return jnp.where(keep, first, second), jnp.where(keep, third, jnp.zeros_like(third))

    for bx in range(3):
        for by in range(3):
            for pair in range(4):
                spots = [(half, bx * 8 + pair * 2 + half - 3) for half in range(2)]
                spots = [(half, at) for half, at in spots if 0 <= at < 18]
                if not spots:
                    continue
                tiles = tiles_of(bx, by, pair * C, C)
                for half, at in spots:
                    for k, value in enumerate(face_pair(tiles, half)):
                        s.near[by, at * C:(at + 1) * C, k * 128:(k + 1) * 128] = value
            tiles = tiles_of(bx, by, 4 * C, 16)
            for half in range(2):
                at = bx * 2 + half
                for k, value in enumerate(face_pair(tiles, half)):
                    s.near_t[by, at * 16:(at + 1) * 16, k * 128:(k + 1) * 128] = value

    wanted = [dot32(s.near_t[by], s.pick_ref[:, 128:256]) for by in range(3)]
    for by in range(3):
        s.faces[by] = dot32(s.near[by], s.pick_ref[...]).astype(BF)

    def window(plane_24, start):
        return pltpu.roll(plane_24, 384 - start, 1)[:, :LANES]

    @pl.loop(0, 18)
    def _(at):
        rows = pl.ds(pl.multiple_of(at * C, 16), C)
        for c in range(3):
            tall = jnp.concatenate([s.faces[by, rows, c * 128:(c + 1) * 128] for by in range(3)], axis=1)
            for b in range(3):
                s.wide1[(b * 3 + c) * C:(b * 3 + c + 1) * C, plane(at)] = window(tall, 48 + 16 * b)

    for at in range(6):
        tall = window(jnp.concatenate([one[at * 16:(at + 1) * 16] for one in wanted], axis=1), 64)
        for pair in range(4):
            xo = (at // 2 - 1) * 8 + pair * 2 + at % 2 + 4
            if 2 <= xo < 14:
                s.want[0:3, plane(xo - 2)] = tall[pair * 4:pair * 4 + 3]

    lane = lax.broadcasted_iota(jnp.int32, (1, LANES), 1)
    y, z = lane >> 4, lane & 15
    region = ((y + 4) >> 3) * 3 + ((z + 4) >> 3)
    inner = jnp.where((y >= 2) & (y < 14) & (z >= 2) & (z < 14), 1.0, 0.0)
    own_lane = jnp.where((y >= 4) & (y < 12) & (z >= 4) & (z < 12), 1.0, 0.0)
    for bx in range(3):
        row = jnp.zeros((1, LANES), F32)
        for j in range(9):
            row = jnp.where(region == j, present[bx * 9 + j], row)
        s.mask_ref[bx, 0:1, :] = row
        for xo in range(2, 14):
            if (xo + 4) // 8 == bx:
                s.mask2[0:1, plane(xo - 2)] = row * inner
                s.mask2[1:2, plane(xo - 2)] = own_lane if bx == 1 else jnp.zeros_like(own_lane)

    s.out1[...] = dot32(s.w1_ref[...], s.wide1[...])

    def first_plane(xo, carry):
        pre = s.out1[0:C, plane(xo)] + s.out1[C:2 * C, plane(xo + 1)] + s.out1[2 * C:3 * C, plane(xo + 2)]
        s.pre1[xo] = pre
        act, _slope = elu_pair(pre)
        hid = (act * s.mask_ref[lax.div(xo + 4, 8), 0:1, :]).astype(BF)
        for bc in range(9):
            shift = -(32 * (bc // 3 - 1) + 2 * (bc % 3 - 1)) % LANES
            s.wide2[bc * C:(bc + 1) * C, plane(xo)] = pltpu.roll(hid, shift, 1) if shift else hid
        return carry

    lax.fori_loop(0, 16, first_plane, 0, unroll=2)

    s.out2[...] = dot32(s.w2_ref[...], s.wide2[...])

    def second_plane(i, carry):
        pre = s.out2[0:C, plane(i)] + s.out2[C:2 * C, plane(i + 2)] + s.out2[2 * C:3 * C, plane(i + 4)]
        act, slope = elu_pair(pre)
        mask = s.mask2[0:1, plane(i)]
        s.hid2[:, plane(i)] = (act * mask).astype(BF)
        s.slope2[:, plane(i)] = slope * mask
        return carry

    lax.fori_loop(0, 12, second_plane, 0, unroll=2)
    logits = dot32(head, s.hid2[...])
    for x in range(8):
        s.raw_logits[x * 8:(x + 1) * 8, :] = logits[0:8, (x + 2) * LANES:(x + 3) * LANES]
    grad_logit = (jax.nn.sigmoid(logits) - s.want[...]) * s.mask2[0:1, :] * scale
    own_logit = (grad_logit * s.mask2[1:2, :]).astype(BF)
    s.back2[...] = dot32(head_t, grad_logit.astype(BF))
    head_grad = lax.dot_general(own_logit, s.hid2[...], NT, preferred_element_type=F32)

    def grad_plane(i, is_own):
        grad_pre = (s.back2[:, plane(i)] * s.slope2[:, plane(i)]).astype(BF)
        for bc in range(9):
            shift = (32 * (bc // 3 - 1) + 2 * (bc % 3 - 1)) % LANES
            s.wide_b[bc * C:(bc + 1) * C, plane(i)] = pltpu.roll(grad_pre, shift, 1) if shift else grad_pre
        if is_own:
            own_pre = (grad_pre.astype(F32) * own_lane).astype(BF)
            for a in range(3):
                s.lhs2[a * C:(a + 1) * C, plane(i + 2 * a - 2)] = own_pre

    def own_plane(i, carry):
        grad_plane(i + 2, True)
        return carry

    lax.fori_loop(0, 8, own_plane, 0, unroll=2)
    for i in (0, 1, 10, 11):
        grad_plane(i, False)

    pack_grads(s.grads_ref, 1, lax.dot_general(
        s.lhs2[...], s.wide2[:, 2 * LANES:14 * LANES], NT, preferred_element_type=F32), jnp.zeros((16, C), F32))
    s.out_b[...] = lax.dot_general(s.wb_ref[...], s.wide_b[...], TN, preferred_element_type=F32)

    @pl.loop(4, 12)
    def _(q):
        back = s.out_b[0:C, plane(q)] + s.out_b[C:2 * C, plane(q - 2)] + s.out_b[2 * C:3 * C, plane(q - 4)]
        _act, slope = elu_pair(s.pre1[q])
        grad_pre = (back * slope * own_lane).astype(BF)
        for a in range(3):
            s.lhs1[a * C:(a + 1) * C, plane(q + a - 4)] = grad_pre

    pack_grads(s.grads_ref, 0, lax.dot_general(
        s.lhs1[...], s.wide1[:, 4 * LANES:14 * LANES], NT, preferred_element_type=F32), head_grad)


def finish_logits(s, logits_ref):
    high = s.raw_logits[...].astype(BF)
    rest = s.raw_logits[...] - high.astype(F32)
    middle = rest.astype(BF)
    low = (rest - middle.astype(F32)).astype(BF)
    cell = lax.broadcasted_iota(jnp.int32, (1, 64), 1)
    source = ((cell >> 3) + 4) * 16 + (cell & 7) + 4
    pick = jnp.where(lax.broadcasted_iota(jnp.int32, (LANES, 64), 0) == source, 1.0, 0.0).astype(BF)
    parts = dot32(jnp.concatenate([high, middle, low], axis=0), pick)
    own_logits = (parts[0:64] + parts[64:128]) + parts[128:192]
    for x in range(8):
        logits_ref[:, x * 64:(x + 1) * 64] = own_logits[x * 8:x * 8 + 3]


def grad_sum_stage(s, g_ref, first_ref, second_ref, head_ref, meanwhile):
    pair_out, pair_in, send_buf, rs_buf, y_buf, done = (
        s.pair_out, s.pair_in, s.send_buf, s.rs_buf, s.y_buf, s.done)
    pair_send, pair_sem, rs_send, rs_sem = s.pair_send, s.pair_sem, s.rs_send, s.rs_sem
    y_send, y_sem, ag_send, ag_sem, last_send, last_sem = (
        s.y_send, s.y_sem, s.ag_send, s.ag_sem, s.last_send, s.last_sem)
    dp, sp = lax.axis_index("dp"), lax.axis_index("space")
    core, y = lax.rem(dp, 2), lax.div(dp, 2)
    n_y, n_sp = y_buf.shape[0], rs_buf.shape[0]
    partner = (dp + 1 - 2 * core, sp)

    def along(r):
        return lax.rem(sp + r, n_sp)

    def line(r):
        return (lax.rem(y + r, n_y) * 2 + core, sp)

    pair_out[...] = g_ref[1 - core].astype(BF)

    def remote(source, target, send, receive, device):
        return pltpu.make_async_remote_copy(
            src_ref=source, dst_ref=target, send_sem=send, recv_sem=receive, device_id=device, device_id_type=MESH)

    pair_copy = remote(pair_out, pair_in, pair_send, pair_sem, partner)
    pair_copy.start()
    pair_copy.wait_recv()
    send_buf[...] = (g_ref[core] + pair_in[...].astype(F32)).astype(BF)

    def rs_copy(r):
        return remote(send_buf.at[along(r)], rs_buf.at[r], rs_send.at[r], rs_sem.at[r], (dp, along(r)))

    def y_copy(r):
        return remote(y_buf.at[0], y_buf.at[r], y_send.at[r], y_sem.at[r], line(r))

    def ag_copy(r):
        return remote(done.at[core, sp], done.at[core, sp], ag_send.at[r], ag_sem.at[r], (dp, along(r)))

    def last_copy(r):
        slot = lax.rem(sp - r + n_sp, n_sp)
        return remote(done.at[core, slot], done.at[core, slot], last_send.at[r], last_sem.at[r], partner)

    for r in range(1, n_sp):
        rs_copy(r).start()
    meanwhile()
    total = g_ref[core, sp] + pair_in[sp].astype(F32)
    for r in range(1, n_sp):
        rs_copy(r).wait_recv()
        total = total + rs_buf[r].astype(F32)
    y_buf[0] = total.astype(BF)
    for r in range(1, n_y):
        y_copy(r).start()
    for r in range(1, n_y):
        y_copy(r).wait_recv()
    total = jnp.zeros(total.shape, F32)
    for d in range(n_y):
        total = total + y_buf[lax.rem(y - d + n_y, n_y)].astype(F32)
    done[core, sp] = total.astype(BF)
    for r in range(1, n_sp):
        ag_copy(r).start()
    last_copy(0).start()
    for r in range(1, n_sp):
        slot = lax.rem(sp - r + n_sp, n_sp)
        remote(done.at[core, slot], done.at[core, slot], ag_send.at[r], ag_sem.at[r], (dp, along(r))).wait_recv()
        last_copy(r).start()
    for r in range(n_sp):
        slot = lax.rem(sp - r + n_sp, n_sp)
        remote(done.at[1 - core, slot], done.at[1 - core, slot], last_send.at[r], last_sem.at[r], partner).wait_recv()

    for part, out in enumerate((first_ref, second_ref)):
        for group in range(9):
            a, rows = group // 3, slice(group % 3 * 16, group % 3 * 16 + 16)
            tail = done[part, 27 + group // 2].astype(F32)
            out[a * 9 + 8, rows, :] = tail[:, 64 * (group % 2):64 * (group % 2) + C]
            wide = jnp.concatenate([done[part, group * 3 + col].astype(F32) for col in range(3)], axis=1)
            for bc in range(8):
                out[a * 9 + bc, rows, :] = wide[:, bc * C:(bc + 1) * C]
    head_ref[...] = done[0, 31].astype(F32)[0:3, 64:64 + C]

    pair_copy.wait_send()
    for r in range(1, n_sp):
        rs_copy(r).wait_send()
        ag_copy(r).wait_send()
    for r in range(1, n_y):
        y_copy(r).wait_send()
    for r in range(n_sp):
        last_copy(r).wait_send()


SCRATCH = dict(
    table=pltpu.SMEM((32,), jnp.int32),
    got=pltpu.VMEM((32, 4 * C + 16, 128), BF), own=pltpu.VMEM((4 * C + 16, 128), BF), wants=pltpu.VMEM((16, 128), F32),
    near=pltpu.VMEM((3, 18 * C, LANES), BF), near_t=pltpu.VMEM((3, 96, LANES), BF),
    faces=pltpu.VMEM((3, 18 * C, 3 * 128), BF), pick_ref=pltpu.VMEM((LANES, 3 * 128), BF),
    wide1=pltpu.VMEM((9 * C, 18 * LANES), BF), out1=pltpu.VMEM((3 * C, 18 * LANES), F32),
    pre1=pltpu.VMEM((16, C, LANES), F32),
    wide2=pltpu.VMEM((9 * C, 16 * LANES), BF), out2=pltpu.VMEM((3 * C, 16 * LANES), F32),
    wide_b=pltpu.VMEM((9 * C, 12 * LANES), BF), out_b=pltpu.VMEM((3 * C, 12 * LANES), F32),
    lhs2=pltpu.VMEM((3 * C, 12 * LANES), BF), lhs1=pltpu.VMEM((3 * C, 10 * LANES), BF),
    want=pltpu.VMEM((16, 12 * LANES), F32), mask_ref=pltpu.VMEM((3, 8, LANES), F32),
    mask2=pltpu.VMEM((8, 12 * LANES), F32), hid2=pltpu.VMEM((C, 12 * LANES), BF),
    slope2=pltpu.VMEM((C, 12 * LANES), F32), back2=pltpu.VMEM((C, 12 * LANES), F32),
    w1_ref=pltpu.VMEM((3 * C, 9 * C), BF), w2_ref=pltpu.VMEM((3 * C, 9 * C), BF),
    wb_ref=pltpu.VMEM((9 * C, 3 * C), BF), head_ref=pltpu.VMEM((16, C), F32),
    raw_logits=pltpu.VMEM((64, LANES), F32), grads_ref=pltpu.VMEM((2, 32, 16, 128), F32),
    pair_out=pltpu.VMEM((32, 16, 128), BF), pair_in=pltpu.VMEM((32, 16, 128), BF),
    send_buf=pltpu.VMEM((32, 16, 128), BF), rs_buf=pltpu.VMEM((32, 16, 128), BF),
    y_buf=pltpu.VMEM((N_Y, 16, 128), BF), done=pltpu.VMEM((2, 32, 16, 128), BF),
    send_sem=pltpu.SemaphoreType.DMA((64,)), recv_sem=pltpu.SemaphoreType.DMA((2, 32)),
    pair_send=pltpu.SemaphoreType.DMA, pair_sem=pltpu.SemaphoreType.DMA,
    rs_send=pltpu.SemaphoreType.DMA((32,)), rs_sem=pltpu.SemaphoreType.DMA((32,)),
    y_send=pltpu.SemaphoreType.DMA((N_Y,)), y_sem=pltpu.SemaphoreType.DMA((N_Y,)),
    ag_send=pltpu.SemaphoreType.DMA((32,)), ag_sem=pltpu.SemaphoreType.DMA((32,)),
    last_send=pltpu.SemaphoreType.DMA((32,)), last_sem=pltpu.SemaphoreType.DMA((32,)),
)


def whole_kernel(scale, ids_ref, features_ref, targets_ref, k1_ref, k2_ref, head_in_ref,
                 logits_ref, first_ref, second_ref, head_out_ref, *scratch):
    s = SimpleNamespace(**dict(zip(SCRATCH, scratch)))
    sent = gather_stage(
        features_ref, targets_ref, s.got, s.own, s.wants, s.send_sem, s.recv_sem,
        lambda: prepare(s, ids_ref, k1_ref, k2_ref, head_in_ref))
    compute(s, scale)
    grad_sum_stage(s, s.grads_ref, first_ref, second_ref, head_out_ref, lambda: finish_logits(s, logits_ref))
    for one in sent:
        one.wait_send()


def on_device(features, device_block, conv_first, conv_second, head_weight, targets):
    n_dp, n_sp = lax.axis_size("dp"), lax.axis_size("space")
    scale = (n_dp * n_sp * 3 * 512) ** (-0.5)
    vmem = pl.BlockSpec(memory_space=pltpu.VMEM)
    kernel = jax.ShapeDtypeStruct((27, C, C), F32)
    logits, first, second, head = pl.pallas_call(
        functools.partial(whole_kernel, scale),
        out_shape=(jax.ShapeDtypeStruct((3, 512), F32), kernel, kernel, jax.ShapeDtypeStruct((3, C), F32)),
        in_specs=[pl.BlockSpec(memory_space=pltpu.SMEM)] + [vmem] * 5,
        out_specs=(vmem,) * 4,
        scratch_shapes=list(SCRATCH.values()),
        compiler_params=pltpu.CompilerParams(
            collective_id=0, has_side_effects=True, vmem_limit_bytes=60 * 1024 * 1024),
    )(device_block, features, targets, conv_first.transpose(1, 0, 2), conv_second.transpose(1, 0, 2), head_weight)
    return (logits[None, None], first.transpose(1, 0, 2), second.transpose(1, 0, 2), head)


def solution(mesh):
    in_specs = (
        P("dp", "space", None, None),
        P("dp", None),
        P(),
        P(),
        P(),
        P("dp", "space", None, None),
    )
    out_specs = (P("dp", "space", None, None), P(), P(), P())
    return jax.shard_map(
        on_device, mesh=mesh, in_specs=in_specs, out_specs=out_specs, check_vma=False
    )
```

```python
import functools
from types import SimpleNamespace

import jax
import jax.numpy as jnp
from jax import lax
from jax.experimental import pallas as pl
from jax.experimental.pallas import tpu as pltpu
from jax.sharding import PartitionSpec as P

BF = jnp.bfloat16
F32 = jnp.float32
C = 48
LANES = 256
NT = (((1,), (1,)), ((), ()))
TN = (((0,), (0,)), ((), ()))


def dot32(a, b):
    return jnp.dot(a, b, preferred_element_type=F32)


def elu_pair(values):
    negative = jnp.exp(jnp.minimum(values, 0.0))
    return (jnp.where(values > 0, values, negative - 1.0), jnp.where(values > 0, 1.0, negative))


def plane(index):
    start = index * LANES
    return pl.ds(start if isinstance(index, int) else pl.multiple_of(start, LANES), LANES)


def pack_grads(grads_ref, part, grads, head):
    for group in range(9):
        rows = grads[group * 16:(group + 1) * 16]
        for col in range(3):
            grads_ref[part, group * 3 + col] = rows[:, col * 128:(col + 1) * 128]
        grads_ref[part, 27 + group // 2, :, 64 * (group % 2):64 * (group % 2) + C] = rows[:, 384:9 * C]
    grads_ref[part, 31, :, 64:64 + C] = head


MESH = pl.DeviceIdType.MESH
N_Z, N_X, N_Y = 8, 4, 8
SPLIT = 48
Z_STEPS = (1, -1, 2, -2, 3, -3, 4)
X_STEPS = (1, -1, 2)


def gather_stage(features_ref, targets_ref, got_ref, own_ref, wants, send_sem, recv_sem, meanwhile):
    dp, sp = lax.axis_index("dp"), lax.axis_index("space")
    z, x = lax.div(sp, N_X), lax.rem(sp, N_X)

    def at(dz, dx):
        return lax.rem(z + dz + N_Z, N_Z) * N_X + lax.rem(x + dx + N_X, N_X)

    near_by = [(dz, 0) for dz in Z_STEPS] + [(0, dx) for dx in X_STEPS]
    barrier = pltpu.get_barrier_semaphore()
    for dz, dx in near_by:
        pl.semaphore_signal(barrier, inc=1, device_id=(dp, at(dz, dx)), device_id_type=MESH)
    others = [(dp + 1 - 2 * lax.rem(dp, 2), sp)] + [(lax.rem(dp + 2 * r, N_Y * 2), sp) for r in range(1, N_Y)]
    for other in others:
        pl.semaphore_signal(barrier, inc=1, device_id=other, device_id_type=MESH)

    wants[...] = jnp.zeros_like(wants)
    for pair in range(4):
        lanes = slice(pair * 128, (pair + 1) * 128)
        own_ref[pair * C:(pair + 1) * C, :] = features_ref[0, 0, :, lanes]
        for j in range(3):
            wants[pair * 4 + j:pair * 4 + j + 1, :] = targets_ref[j * 4 + pair:j * 4 + pair + 1, :].astype(F32)
    own_ref[4 * C:4 * C + 16, :] = wants[...].astype(BF)
    got_ref[sp] = own_ref[...]
    pl.semaphore_wait(barrier, len(near_by) + len(others))

    rows = [pl.ds(0, SPLIT), pl.ds(SPLIT, own_ref.shape[0] - SPLIT)]
    sent = []

    def copy(half, dz, dx, to, number):
        slot = at(dz, dx)
        source = own_ref.at[rows[half]] if (dz, dx) == (0, 0) else got_ref.at[slot, rows[half]]
        return pltpu.make_async_remote_copy(
            src_ref=source, dst_ref=got_ref.at[slot, rows[half]], send_sem=send_sem.at[number],
            recv_sem=recv_sem.at[half, slot], device_id=(dp, at(*to)), device_id_type=MESH)

    def send(half, dz, dx, to):
        one = copy(half, dz, dx, to, len(sent))
        one.start()
        sent.append(one)

    arrived = set()

    def await_block(half, dz, dx):
        if (half, dz, dx) in arrived:
            return
        arrived.add((half, dz, dx))
        slot = at(dz, dx)
        pltpu.make_async_remote_copy(
            src_ref=own_ref.at[rows[half]], dst_ref=got_ref.at[slot, rows[half]], send_sem=send_sem.at[0],
            recv_sem=recv_sem.at[half, slot], device_id=(dp, at(0, 1)), device_id_type=MESH).wait_recv()

    for dx in X_STEPS:
        send(0, 0, 0, (0, dx))
    for dz in Z_STEPS:
        send(1, 0, 0, (dz, 0))
    for dx in X_STEPS:
        send(1, 0, 0, (0, dx))
    for dz in Z_STEPS:
        send(0, 0, 0, (dz, 0))
    meanwhile()

    def pass_x(dx):
        await_block(0, 0, dx)
        for dz in Z_STEPS:
            send(0, 0, dx, (dz, 0))

    def pass_z(dz):
        await_block(1, dz, 0)
        for dx in X_STEPS:
            send(1, dz, 0, (0, dx))

    for dz in (1, -1):
        pass_z(dz)
    for dx in X_STEPS:
        pass_x(dx)
    for dz in (2, -2, 3, -3, 4):
        pass_z(dz)
    for dz in Z_STEPS:
        for dx in (0, *X_STEPS):
            await_block(0, dz, dx)
    for dz in (0, *Z_STEPS):
        for dx in X_STEPS:
            await_block(1, dz, dx)
    return sent


def prepare(s, ids_ref, k1_ref, k2_ref, head_in_ref):
    for t in range(27):
        a, bc = t // 9, t % 9
        s.w1_ref[a * C:(a + 1) * C, bc * C:(bc + 1) * C] = k1_ref[t]
        s.w2_ref[a * C:(a + 1) * C, bc * C:(bc + 1) * C] = k2_ref[t]
        s.wb_ref[bc * C:(bc + 1) * C, a * C:(a + 1) * C] = k2_ref[t]
    s.head_ref[...] = jnp.zeros_like(s.head_ref)
    s.head_ref[0:3, :] = head_in_ref[...].astype(F32)

    column = lax.broadcasted_iota(jnp.int32, (1, 3 * 128), 1)
    z = (column & 15) + (column >> 7) + 3
    source = (z >> 3) * 64 + ((column >> 4) & 7) * 8 + (z & 7)
    s.pick_ref[...] = jnp.where(lax.broadcasted_iota(jnp.int32, (LANES, 3 * 128), 0) == source, 1.0, 0.0).astype(BF)
    for ref in (s.want, s.lhs2, s.lhs1):
        ref[...] = jnp.zeros_like(ref)
    s.grads_ref[:, 27:32] = jnp.zeros((2, 5, 16, 128), F32)

    own = ids_ref[0, lax.axis_index("space")]
    ox, oy, oz = own // 16, own // 4 % 4, own % 4

    @pl.loop(0, 27)
    def _(t):
        x, y, z = ox + t // 9 - 1, oy + t // 3 % 3 - 1, oz + t % 3 - 1
        inside = (x >= 0) & (x < 4) & (y >= 0) & (y < 4) & (z >= 0) & (z < 4)
        wanted = jnp.where(inside, (x * 4 + y) * 4 + z, -1)
        found = jnp.int32(-1)
        for j in range(32):
            found = jnp.where(ids_ref[0, j] == wanted, j, found)
        s.table[t] = found


def compute(s, scale):
    slots = [jnp.maximum(s.table[t], 0) for t in range(27)]
    present = [jnp.where(s.table[t] >= 0, 1.0, 0.0).astype(F32) for t in range(27)]
    head = s.head_ref[...].astype(BF)
    head_t = s.head_ref[...].T.astype(BF)

    low_half = lax.broadcasted_iota(jnp.int32, (C, 128), 1) < 64

    def tiles_of(bx, by, row, rows):
        return [
            (s.got[slots[t], row:row + rows, :].astype(F32) * present[t]).astype(BF)
            for t in (bx * 9 + by * 3 + bz for bz in range(3))
        ]

    def face_pair(tiles, half):
        keep = low_half[:tiles[0].shape[0]]
        flip = lambda v: pltpu.roll(v, 64, 1)
        first = tiles[0] if half == 0 else flip(tiles[0])
        second = tiles[1] if half == 1 else flip(tiles[1])
        third = tiles[2] if half == 0 else flip(tiles[2])
        return jnp.where(keep, first, second), jnp.where(keep, third, jnp.zeros_like(third))

    for bx in range(3):
        for by in range(3):
            for pair in range(4):
                spots = [(half, bx * 8 + pair * 2 + half - 3) for half in range(2)]
                spots = [(half, at) for half, at in spots if 0 <= at < 18]
                if not spots:
                    continue
                tiles = tiles_of(bx, by, pair * C, C)
                for half, at in spots:
                    for k, value in enumerate(face_pair(tiles, half)):
                        s.near[by, at * C:(at + 1) * C, k * 128:(k + 1) * 128] = value
            tiles = tiles_of(bx, by, 4 * C, 16)
            for half in range(2):
                at = bx * 2 + half
                for k, value in enumerate(face_pair(tiles, half)):
                    s.near_t[by, at * 16:(at + 1) * 16, k * 128:(k + 1) * 128] = value

    wanted = [dot32(s.near_t[by], s.pick_ref[:, 128:256]) for by in range(3)]
    for by in range(3):
        s.faces[by] = dot32(s.near[by], s.pick_ref[...]).astype(BF)

    def window(plane_24, start):
        return pltpu.roll(plane_24, 384 - start, 1)[:, :LANES]

    def window_plane(at, carry):
        rows = pl.ds(pl.multiple_of(at * C, 16), C)
        for c in range(3):
            tall = jnp.concatenate([s.faces[by, rows, c * 128:(c + 1) * 128] for by in range(3)], axis=1)
            for b in range(3):
                s.wide1[(b * 3 + c) * C:(b * 3 + c + 1) * C, plane(at)] = window(tall, 48 + 16 * b)
        return carry

    lax.fori_loop(0, 18, window_plane, 0, unroll=3)

    for at in range(6):
        tall = window(jnp.concatenate([one[at * 16:(at + 1) * 16] for one in wanted], axis=1), 64)
        for pair in range(4):
            xo = (at // 2 - 1) * 8 + pair * 2 + at % 2 + 4
            if 2 <= xo < 14:
                s.want[0:3, plane(xo - 2)] = tall[pair * 4:pair * 4 + 3]

    lane = lax.broadcasted_iota(jnp.int32, (1, LANES), 1)
    y, z = lane >> 4, lane & 15
    region = ((y + 4) >> 3) * 3 + ((z + 4) >> 3)
    inner = jnp.where((y >= 2) & (y < 14) & (z >= 2) & (z < 14), 1.0, 0.0)
    own_lane = jnp.where((y >= 4) & (y < 12) & (z >= 4) & (z < 12), 1.0, 0.0)
    for bx in range(3):
        row = jnp.zeros((1, LANES), F32)
        for j in range(9):
            row = jnp.where(region == j, present[bx * 9 + j], row)
        s.mask_ref[bx, 0:1, :] = row
        for xo in range(2, 14):
            if (xo + 4) // 8 == bx:
                s.mask2[0:1, plane(xo - 2)] = row * inner
                s.mask2[1:2, plane(xo - 2)] = own_lane if bx == 1 else jnp.zeros_like(own_lane)

    s.out1[...] = dot32(s.w1_ref[...], s.wide1[...])

    def first_plane(xo, carry):
        pre = s.out1[0:C, plane(xo)] + s.out1[C:2 * C, plane(xo + 1)] + s.out1[2 * C:3 * C, plane(xo + 2)]
        s.pre1[xo] = pre
        act, _slope = elu_pair(pre)
        hid = (act * s.mask_ref[lax.div(xo + 4, 8), 0:1, :]).astype(BF)
        for bc in range(9):
            shift = -(32 * (bc // 3 - 1) + 2 * (bc % 3 - 1)) % LANES
            s.wide2[bc * C:(bc + 1) * C, plane(xo)] = pltpu.roll(hid, shift, 1) if shift else hid
        return carry

    lax.fori_loop(0, 16, first_plane, 0, unroll=4)

    s.out2[...] = dot32(s.w2_ref[...], s.wide2[...])

    def second_plane(i, carry):
        pre = s.out2[0:C, plane(i)] + s.out2[C:2 * C, plane(i + 2)] + s.out2[2 * C:3 * C, plane(i + 4)]
        act, slope = elu_pair(pre)
        mask = s.mask2[0:1, plane(i)]
        s.hid2[:, plane(i)] = (act * mask).astype(BF)
        s.slope2[:, plane(i)] = slope * mask
        return carry

    lax.fori_loop(0, 12, second_plane, 0, unroll=4)
    logits = dot32(head, s.hid2[...])
    for x in range(8):
        s.raw_logits[x * 8:(x + 1) * 8, :] = logits[0:8, (x + 2) * LANES:(x + 3) * LANES]
    grad_logit = (jax.nn.sigmoid(logits) - s.want[...]) * s.mask2[0:1, :] * scale
    own_logit = (grad_logit * s.mask2[1:2, :]).astype(BF)
    s.back2[...] = dot32(head_t, grad_logit.astype(BF))
    head_grad = lax.dot_general(own_logit, s.hid2[...], NT, preferred_element_type=F32)

    def grad_plane(i, is_own):
        grad_pre = (s.back2[:, plane(i)] * s.slope2[:, plane(i)]).astype(BF)
        for bc in range(9):
            shift = (32 * (bc // 3 - 1) + 2 * (bc % 3 - 1)) % LANES
            s.wide_b[bc * C:(bc + 1) * C, plane(i)] = pltpu.roll(grad_pre, shift, 1) if shift else grad_pre
        if is_own:
            own_pre = (grad_pre.astype(F32) * own_lane).astype(BF)
            for a in range(3):
                s.lhs2[a * C:(a + 1) * C, plane(i + 2 * a - 2)] = own_pre

    def own_plane(i, carry):
        grad_plane(i + 2, True)
        return carry

    lax.fori_loop(0, 8, own_plane, 0, unroll=4)
    for i in (0, 1, 10, 11):
        grad_plane(i, False)

    pack_grads(s.grads_ref, 1, lax.dot_general(
        s.lhs2[...], s.wide2[:, 2 * LANES:14 * LANES], NT, preferred_element_type=F32), jnp.zeros((16, C), F32))
    s.out_b[...] = lax.dot_general(s.wb_ref[...], s.wide_b[...], TN, preferred_element_type=F32)

    def last_plane(q, carry):
        back = s.out_b[0:C, plane(q)] + s.out_b[C:2 * C, plane(q - 2)] + s.out_b[2 * C:3 * C, plane(q - 4)]
        _act, slope = elu_pair(s.pre1[q])
        grad_pre = (back * slope * own_lane).astype(BF)
        for a in range(3):
            s.lhs1[a * C:(a + 1) * C, plane(q + a - 4)] = grad_pre
        return carry

    lax.fori_loop(4, 12, last_plane, 0, unroll=4)

    pack_grads(s.grads_ref, 0, lax.dot_general(
        s.lhs1[...], s.wide1[:, 4 * LANES:14 * LANES], NT, preferred_element_type=F32), head_grad)


def finish_logits(s, logits_ref):
    high = s.raw_logits[...].astype(BF)
    rest = s.raw_logits[...] - high.astype(F32)
    middle = rest.astype(BF)
    low = (rest - middle.astype(F32)).astype(BF)
    cell = lax.broadcasted_iota(jnp.int32, (1, 64), 1)
    source = ((cell >> 3) + 4) * 16 + (cell & 7) + 4
    pick = jnp.where(lax.broadcasted_iota(jnp.int32, (LANES, 64), 0) == source, 1.0, 0.0).astype(BF)
    parts = dot32(jnp.concatenate([high, middle, low], axis=0), pick)
    own_logits = (parts[0:64] + parts[64:128]) + parts[128:192]
    for x in range(8):
        for j in range(3):
            row = j * 4 + x // 2
            logits_ref[row:row + 1, x % 2 * 64:x % 2 * 64 + 64] = own_logits[x * 8 + j:x * 8 + j + 1]


def grad_sum_stage(s, g_ref, first_ref, second_ref, head_ref, meanwhile):
    pair_out, pair_in, send_buf, rs_buf, y_buf, done = (
        s.pair_out, s.pair_in, s.send_buf, s.rs_buf, s.y_buf, s.done)
    pair_send, pair_sem, rs_send, rs_sem = s.pair_send, s.pair_sem, s.rs_send, s.rs_sem
    y_send, y_sem, ag_send, ag_sem, last_send, last_sem = (
        s.y_send, s.y_sem, s.ag_send, s.ag_sem, s.last_send, s.last_sem)
    dp, sp = lax.axis_index("dp"), lax.axis_index("space")
    core, y = lax.rem(dp, 2), lax.div(dp, 2)
    n_y, n_sp = y_buf.shape[0], rs_buf.shape[0]
    partner = (dp + 1 - 2 * core, sp)

    def along(r):
        return lax.rem(sp + r, n_sp)

    def line(r):
        return (lax.rem(y + r, n_y) * 2 + core, sp)

    pair_out[...] = g_ref[1 - core].astype(BF)

    def remote(source, target, send, receive, device):
        return pltpu.make_async_remote_copy(
            src_ref=source, dst_ref=target, send_sem=send, recv_sem=receive, device_id=device, device_id_type=MESH)

    pair_copy = remote(pair_out, pair_in, pair_send, pair_sem, partner)
    pair_copy.start()
    pair_copy.wait_recv()
    send_buf[...] = (g_ref[core] + pair_in[...].astype(F32)).astype(BF)

    far_first = sorted(range(1, n_sp), key=lambda r: abs(n_sp // 2 - r))
    y_far_first = sorted(range(1, n_y), key=lambda r: abs(n_y // 2 - r))

    def rs_copy(r):
        return remote(send_buf.at[along(r)], rs_buf.at[r], rs_send.at[r], rs_sem.at[r], (dp, along(r)))

    def y_copy(r):
        return remote(y_buf.at[0], y_buf.at[r], y_send.at[r], y_sem.at[r], line(r))

    def ag_copy(r):
        return remote(done.at[core, sp], done.at[core, sp], ag_send.at[r], ag_sem.at[r], (dp, along(r)))

    def last_copy(r):
        slot = lax.rem(sp - r + n_sp, n_sp)
        return remote(done.at[core, slot], done.at[core, slot], last_send.at[r], last_sem.at[r], partner)

    for r in far_first:
        rs_copy(r).start()
    meanwhile()
    total = g_ref[core, sp] + pair_in[sp].astype(F32)
    for r in reversed(far_first):
        rs_copy(r).wait_recv()
        total = total + rs_buf[r].astype(F32)
    y_buf[0] = total.astype(BF)
    for r in y_far_first:
        y_copy(r).start()
    for r in range(1, n_y):
        y_copy(r).wait_recv()
    total = jnp.zeros(total.shape, F32)
    for d in range(n_y):
        total = total + y_buf[lax.rem(y - d + n_y, n_y)].astype(F32)
    done[core, sp] = total.astype(BF)
    for r in far_first:
        ag_copy(r).start()
    last_copy(0).start()
    for r in reversed(far_first):
        slot = lax.rem(sp - r + n_sp, n_sp)
        remote(done.at[core, slot], done.at[core, slot], ag_send.at[r], ag_sem.at[r], (dp, along(r))).wait_recv()
        last_copy(r).start()
    for r in range(n_sp):
        slot = lax.rem(sp - r + n_sp, n_sp)
        remote(done.at[1 - core, slot], done.at[1 - core, slot], last_send.at[r], last_sem.at[r], partner).wait_recv()

    for part, out in enumerate((first_ref, second_ref)):
        for group in range(9):
            a, rows = group // 3, slice(group % 3 * 16, group % 3 * 16 + 16)
            tail = done[part, 27 + group // 2]
            out[a * 9 + 8, rows, :] = tail[:, 64 * (group % 2):64 * (group % 2) + C]
            wide = jnp.concatenate([done[part, group * 3 + col] for col in range(3)], axis=1)
            for bc in range(8):
                out[a * 9 + bc, rows, :] = wide[:, bc * C:(bc + 1) * C]
    head_ref[...] = done[0, 31].astype(F32)[0:3, 64:64 + C]

    pair_copy.wait_send()
    for r in range(1, n_sp):
        rs_copy(r).wait_send()
        ag_copy(r).wait_send()
    for r in range(1, n_y):
        y_copy(r).wait_send()
    for r in range(n_sp):
        last_copy(r).wait_send()


SCRATCH = dict(
    table=pltpu.SMEM((32,), jnp.int32),
    got=pltpu.VMEM((32, 4 * C + 16, 128), BF), own=pltpu.VMEM((4 * C + 16, 128), BF), wants=pltpu.VMEM((16, 128), F32),
    near=pltpu.VMEM((3, 18 * C, LANES), BF), near_t=pltpu.VMEM((3, 96, LANES), BF),
    faces=pltpu.VMEM((3, 18 * C, 3 * 128), BF), pick_ref=pltpu.VMEM((LANES, 3 * 128), BF),
    wide1=pltpu.VMEM((9 * C, 18 * LANES), BF), out1=pltpu.VMEM((3 * C, 18 * LANES), F32),
    pre1=pltpu.VMEM((16, C, LANES), F32),
    wide2=pltpu.VMEM((9 * C, 16 * LANES), BF), out2=pltpu.VMEM((3 * C, 16 * LANES), F32),
    wide_b=pltpu.VMEM((9 * C, 12 * LANES), BF), out_b=pltpu.VMEM((3 * C, 12 * LANES), F32),
    lhs2=pltpu.VMEM((3 * C, 12 * LANES), BF), lhs1=pltpu.VMEM((3 * C, 10 * LANES), BF),
    want=pltpu.VMEM((16, 12 * LANES), F32), mask_ref=pltpu.VMEM((3, 8, LANES), F32),
    mask2=pltpu.VMEM((8, 12 * LANES), F32), hid2=pltpu.VMEM((C, 12 * LANES), BF),
    slope2=pltpu.VMEM((C, 12 * LANES), F32), back2=pltpu.VMEM((C, 12 * LANES), F32),
    w1_ref=pltpu.VMEM((3 * C, 9 * C), BF), w2_ref=pltpu.VMEM((3 * C, 9 * C), BF),
    wb_ref=pltpu.VMEM((9 * C, 3 * C), BF), head_ref=pltpu.VMEM((16, C), F32),
    raw_logits=pltpu.VMEM((64, LANES), F32), grads_ref=pltpu.VMEM((2, 32, 16, 128), F32),
    pair_out=pltpu.VMEM((32, 16, 128), BF), pair_in=pltpu.VMEM((32, 16, 128), BF),
    send_buf=pltpu.VMEM((32, 16, 128), BF), rs_buf=pltpu.VMEM((32, 16, 128), BF),
    y_buf=pltpu.VMEM((N_Y, 16, 128), BF), done=pltpu.VMEM((2, 32, 16, 128), BF),
    send_sem=pltpu.SemaphoreType.DMA((64,)), recv_sem=pltpu.SemaphoreType.DMA((2, 32)),
    pair_send=pltpu.SemaphoreType.DMA, pair_sem=pltpu.SemaphoreType.DMA,
    rs_send=pltpu.SemaphoreType.DMA((32,)), rs_sem=pltpu.SemaphoreType.DMA((32,)),
    y_send=pltpu.SemaphoreType.DMA((N_Y,)), y_sem=pltpu.SemaphoreType.DMA((N_Y,)),
    ag_send=pltpu.SemaphoreType.DMA((32,)), ag_sem=pltpu.SemaphoreType.DMA((32,)),
    last_send=pltpu.SemaphoreType.DMA((32,)), last_sem=pltpu.SemaphoreType.DMA((32,)),
)


def whole_kernel(scale, ids_ref, features_ref, targets_ref, k1_ref, k2_ref, head_in_ref,
                 logits_ref, first_ref, second_ref, head_out_ref, *scratch):
    s = SimpleNamespace(**dict(zip(SCRATCH, scratch)))
    sent = gather_stage(
        features_ref, targets_ref, s.got, s.own, s.wants, s.send_sem, s.recv_sem,
        lambda: prepare(s, ids_ref, k1_ref, k2_ref, head_in_ref))
    compute(s, scale)
    grad_sum_stage(s, s.grads_ref, first_ref, second_ref, head_out_ref, lambda: finish_logits(s, logits_ref))
    for one in sent:
        one.wait_send()


def on_device(features, device_block, conv_first, conv_second, head_weight, targets):
    n_dp, n_sp = lax.axis_size("dp"), lax.axis_size("space")
    scale = (n_dp * n_sp * 3 * 512) ** (-0.5)
    vmem = pl.BlockSpec(memory_space=pltpu.VMEM)
    kernel = jax.ShapeDtypeStruct((27, C, C), BF)
    logits, first, second, head = pl.pallas_call(
        functools.partial(whole_kernel, scale),
        out_shape=(jax.ShapeDtypeStruct((12, 128), F32), kernel, kernel, jax.ShapeDtypeStruct((3, C), F32)),
        in_specs=[pl.BlockSpec(memory_space=pltpu.SMEM)] + [vmem] * 5,
        out_specs=(vmem,) * 4,
        scratch_shapes=list(SCRATCH.values()),
        compiler_params=pltpu.CompilerParams(
            collective_id=0, has_side_effects=True, vmem_limit_bytes=60 * 1024 * 1024),
    )(device_block, features, targets.reshape(12, 128), conv_first.transpose(1, 0, 2), conv_second.transpose(1, 0, 2), head_weight)
    return (
        logits.reshape(1, 1, 3, 512), first.transpose(1, 0, 2).astype(F32), second.transpose(1, 0, 2).astype(F32), head)


def solution(mesh):
    in_specs = (
        P("dp", "space", None, None),
        P("dp", None),
        P(),
        P(),
        P(),
        P("dp", "space", None, None),
    )
    out_specs = (P("dp", "space", None, None), P(), P(), P())
    return jax.shard_map(
        on_device, mesh=mesh, in_specs=in_specs, out_specs=out_specs, check_vma=False
    )
```

```python
import functools
from types import SimpleNamespace

import jax
import jax.numpy as jnp
from jax import lax
from jax.experimental import pallas as pl
from jax.experimental.pallas import tpu as pltpu
from jax.sharding import PartitionSpec as P

BF = jnp.bfloat16
F32 = jnp.float32
C = 48
LANES = 256
NT = (((1,), (1,)), ((), ()))
TN = (((0,), (0,)), ((), ()))


def dot32(a, b):
    return jnp.dot(a, b, preferred_element_type=F32)


def elu_pair(values):
    negative = jnp.exp(jnp.minimum(values, 0.0))
    return (jnp.where(values > 0, values, negative - 1.0), jnp.where(values > 0, 1.0, negative))


def plane(index):
    start = index * LANES
    return pl.ds(start if isinstance(index, int) else pl.multiple_of(start, LANES), LANES)


def pack_grads(grads_ref, part, grads, head):
    for group in range(9):
        rows = grads[group * 16:(group + 1) * 16]
        for col in range(3):
            grads_ref[part, group * 3 + col] = rows[:, col * 128:(col + 1) * 128]
        grads_ref[part, 27 + group // 2, :, 64 * (group % 2):64 * (group % 2) + C] = rows[:, 384:9 * C]
    grads_ref[part, 31, :, 64:64 + C] = head


MESH = pl.DeviceIdType.MESH
N_Z, N_X, N_Y = 8, 4, 8
SPLIT = 48
Z_STEPS = (1, -1, 2, -2, 3, -3, 4)
X_STEPS = (1, -1, 2)


def gather_stage(features_ref, targets_ref, got_ref, own_ref, wants, send_sem, recv_sem, meanwhile):
    dp, sp = lax.axis_index("dp"), lax.axis_index("space")
    z, x = lax.div(sp, N_X), lax.rem(sp, N_X)

    def at(dz, dx):
        return lax.rem(z + dz + N_Z, N_Z) * N_X + lax.rem(x + dx + N_X, N_X)

    near_by = [(dz, 0) for dz in Z_STEPS] + [(0, dx) for dx in X_STEPS]
    barrier = pltpu.get_barrier_semaphore()
    for dz, dx in near_by:
        pl.semaphore_signal(barrier, inc=1, device_id=(dp, at(dz, dx)), device_id_type=MESH)
    others = [(dp + 1 - 2 * lax.rem(dp, 2), sp)] + [(lax.rem(dp + 2 * r, N_Y * 2), sp) for r in range(1, N_Y)]
    for other in others:
        pl.semaphore_signal(barrier, inc=1, device_id=other, device_id_type=MESH)

    wants[...] = jnp.zeros_like(wants)
    for pair in range(4):
        lanes = slice(pair * 128, (pair + 1) * 128)
        own_ref[pair * C:(pair + 1) * C, :] = features_ref[0, 0, :, lanes]
        for j in range(3):
            wants[pair * 4 + j:pair * 4 + j + 1, :] = targets_ref[j * 4 + pair:j * 4 + pair + 1, :].astype(F32)
    own_ref[4 * C:4 * C + 16, :] = wants[...].astype(BF)
    got_ref[sp] = own_ref[...]
    pl.semaphore_wait(barrier, len(near_by) + len(others))

    rows = [pl.ds(0, SPLIT), pl.ds(SPLIT, own_ref.shape[0] - SPLIT)]
    sent = []

    def copy(half, dz, dx, to, number):
        slot = at(dz, dx)
        source = own_ref.at[rows[half]] if (dz, dx) == (0, 0) else got_ref.at[slot, rows[half]]
        return pltpu.make_async_remote_copy(
            src_ref=source, dst_ref=got_ref.at[slot, rows[half]], send_sem=send_sem.at[number],
            recv_sem=recv_sem.at[half, slot], device_id=(dp, at(*to)), device_id_type=MESH)

    def send(half, dz, dx, to):
        one = copy(half, dz, dx, to, len(sent))
        one.start()
        sent.append(one)

    arrived = set()

    def await_block(half, dz, dx):
        if (half, dz, dx) in arrived:
            return
        arrived.add((half, dz, dx))
        slot = at(dz, dx)
        pltpu.make_async_remote_copy(
            src_ref=own_ref.at[rows[half]], dst_ref=got_ref.at[slot, rows[half]], send_sem=send_sem.at[0],
            recv_sem=recv_sem.at[half, slot], device_id=(dp, at(0, 1)), device_id_type=MESH).wait_recv()

    for dx in X_STEPS:
        send(0, 0, 0, (0, dx))
    for dz in Z_STEPS:
        send(1, 0, 0, (dz, 0))
    for dx in X_STEPS:
        send(1, 0, 0, (0, dx))
    for dz in Z_STEPS:
        send(0, 0, 0, (dz, 0))
    meanwhile()

    def pass_x(dx):
        await_block(0, 0, dx)
        for dz in Z_STEPS:
            send(0, 0, dx, (dz, 0))

    def pass_z(dz):
        await_block(1, dz, 0)
        for dx in X_STEPS:
            send(1, dz, 0, (0, dx))

    for dz in (1, -1):
        pass_z(dz)
    for dx in X_STEPS:
        pass_x(dx)
    for dz in (2, -2, 3, -3, 4):
        pass_z(dz)
    for dz in Z_STEPS:
        for dx in (0, *X_STEPS):
            await_block(0, dz, dx)
    for dz in (0, *Z_STEPS):
        for dx in X_STEPS:
            await_block(1, dz, dx)
    return sent


def prepare(s, ids_ref, k1_ref, k2_ref, head_in_ref):
    for t in range(27):
        a, bc = t // 9, t % 9
        s.w1_ref[a * C:(a + 1) * C, bc * C:(bc + 1) * C] = k1_ref[t]
        s.w2_ref[a * C:(a + 1) * C, bc * C:(bc + 1) * C] = k2_ref[t]
        s.wb_ref[bc * C:(bc + 1) * C, a * C:(a + 1) * C] = k2_ref[t]
    s.head_ref[...] = jnp.zeros_like(s.head_ref)
    s.head_ref[0:3, :] = head_in_ref[...].astype(F32)

    column = lax.broadcasted_iota(jnp.int32, (1, 3 * 128), 1)
    z = (column & 15) + (column >> 7) + 3
    source = (z >> 3) * 64 + ((column >> 4) & 7) * 8 + (z & 7)
    s.pick_ref[...] = jnp.where(lax.broadcasted_iota(jnp.int32, (LANES, 3 * 128), 0) == source, 1.0, 0.0).astype(BF)
    for ref in (s.want, s.lhs2, s.lhs1):
        ref[...] = jnp.zeros_like(ref)
    s.grads_ref[:, 27:32] = jnp.zeros((2, 5, 16, 128), F32)

    own = ids_ref[0, lax.axis_index("space")]
    ox, oy, oz = own // 16, own // 4 % 4, own % 4

    @pl.loop(0, 27)
    def _(t):
        x, y, z = ox + t // 9 - 1, oy + t // 3 % 3 - 1, oz + t % 3 - 1
        inside = (x >= 0) & (x < 4) & (y >= 0) & (y < 4) & (z >= 0) & (z < 4)
        wanted = jnp.where(inside, (x * 4 + y) * 4 + z, -1)
        found = jnp.int32(-1)
        for j in range(32):
            found = jnp.where(ids_ref[0, j] == wanted, j, found)
        s.table[t] = found


def compute(s, scale):
    slots = [jnp.maximum(s.table[t], 0) for t in range(27)]
    present = [jnp.where(s.table[t] >= 0, 1.0, 0.0).astype(F32) for t in range(27)]
    head = s.head_ref[...].astype(BF)
    head_t = s.head_ref[...].T.astype(BF)

    low_half = lax.broadcasted_iota(jnp.int32, (C, 128), 1) < 64

    def tiles_of(bx, by, row, rows):
        return [
            (s.got[slots[t], row:row + rows, :].astype(F32) * present[t]).astype(BF)
            for t in (bx * 9 + by * 3 + bz for bz in range(3))
        ]

    def face_pair(tiles, half):
        keep = low_half[:tiles[0].shape[0]]
        flip = lambda v: pltpu.roll(v, 64, 1)
        first = tiles[0] if half == 0 else flip(tiles[0])
        second = tiles[1] if half == 1 else flip(tiles[1])
        third = tiles[2] if half == 0 else flip(tiles[2])
        return jnp.where(keep, first, second), jnp.where(keep, third, jnp.zeros_like(third))

    for bx in range(3):
        for by in range(3):
            for pair in range(4):
                spots = [(half, bx * 8 + pair * 2 + half - 3) for half in range(2)]
                spots = [(half, at) for half, at in spots if 0 <= at < 18]
                if not spots:
                    continue
                tiles = tiles_of(bx, by, pair * C, C)
                for half, at in spots:
                    for k, value in enumerate(face_pair(tiles, half)):
                        s.near[by, at * C:(at + 1) * C, k * 128:(k + 1) * 128] = value
            tiles = tiles_of(bx, by, 4 * C, 16)
            for half in range(2):
                at = bx * 2 + half
                for k, value in enumerate(face_pair(tiles, half)):
                    s.near_t[by, at * 16:(at + 1) * 16, k * 128:(k + 1) * 128] = value

    wanted = [dot32(s.near_t[by], s.pick_ref[:, 128:256]) for by in range(3)]
    for by in range(3):
        s.faces[by] = dot32(s.near[by], s.pick_ref[...]).astype(BF)

    def window(plane_24, start):
        return pltpu.roll(plane_24, 384 - start, 1)[:, :LANES]

    def window_plane(at, carry):
        rows = pl.ds(pl.multiple_of(at * C, 16), C)
        for c in range(3):
            tall = jnp.concatenate([s.faces[by, rows, c * 128:(c + 1) * 128] for by in range(3)], axis=1)
            for b in range(3):
                s.wide1[(b * 3 + c) * C:(b * 3 + c + 1) * C, plane(at)] = window(tall, 48 + 16 * b)
        return carry

    lax.fori_loop(0, 18, window_plane, 0, unroll=3)

    for at in range(6):
        tall = window(jnp.concatenate([one[at * 16:(at + 1) * 16] for one in wanted], axis=1), 64)
        for pair in range(4):
            xo = (at // 2 - 1) * 8 + pair * 2 + at % 2 + 4
            if 2 <= xo < 14:
                s.want[0:3, plane(xo - 2)] = tall[pair * 4:pair * 4 + 3]

    lane = lax.broadcasted_iota(jnp.int32, (1, LANES), 1)
    y, z = lane >> 4, lane & 15
    region = ((y + 4) >> 3) * 3 + ((z + 4) >> 3)
    inner = jnp.where((y >= 2) & (y < 14) & (z >= 2) & (z < 14), 1.0, 0.0)
    own_lane = jnp.where((y >= 4) & (y < 12) & (z >= 4) & (z < 12), 1.0, 0.0)
    for bx in range(3):
        row = jnp.zeros((1, LANES), F32)
        for j in range(9):
            row = jnp.where(region == j, present[bx * 9 + j], row)
        s.mask_ref[bx, 0:1, :] = row
        for xo in range(2, 14):
            if (xo + 4) // 8 == bx:
                s.mask2[0:1, plane(xo - 2)] = row * inner
                s.mask2[1:2, plane(xo - 2)] = own_lane if bx == 1 else jnp.zeros_like(own_lane)

    s.out1[...] = dot32(s.w1_ref[...], s.wide1[...])

    def first_plane(xo, carry):
        pre = s.out1[0:C, plane(xo)] + s.out1[C:2 * C, plane(xo + 1)] + s.out1[2 * C:3 * C, plane(xo + 2)]
        s.pre1[xo] = pre
        act, _slope = elu_pair(pre)
        hid = (act * s.mask_ref[lax.div(xo + 4, 8), 0:1, :]).astype(BF)
        for bc in range(9):
            shift = -(32 * (bc // 3 - 1) + 2 * (bc % 3 - 1)) % LANES
            s.wide2[bc * C:(bc + 1) * C, plane(xo)] = pltpu.roll(hid, shift, 1) if shift else hid
        return carry

    lax.fori_loop(0, 16, first_plane, 0, unroll=4)

    s.out2[...] = dot32(s.w2_ref[...], s.wide2[...])

    def second_plane(i, carry):
        pre = s.out2[0:C, plane(i)] + s.out2[C:2 * C, plane(i + 2)] + s.out2[2 * C:3 * C, plane(i + 4)]
        act, slope = elu_pair(pre)
        mask = s.mask2[0:1, plane(i)]
        s.hid2[:, plane(i)] = (act * mask).astype(BF)
        s.slope2[:, plane(i)] = slope * mask
        return carry

    lax.fori_loop(0, 12, second_plane, 0, unroll=4)
    logits = dot32(head, s.hid2[...])
    for x in range(8):
        s.raw_logits[x * 8:(x + 1) * 8, :] = logits[0:8, (x + 2) * LANES:(x + 3) * LANES]
    grad_logit = (jax.nn.sigmoid(logits) - s.want[...]) * s.mask2[0:1, :] * scale
    own_logit = (grad_logit * s.mask2[1:2, :]).astype(BF)
    s.back2[...] = dot32(head_t, grad_logit.astype(BF))
    head_grad = lax.dot_general(own_logit, s.hid2[...], NT, preferred_element_type=F32)

    def grad_plane(i, is_own):
        grad_pre = (s.back2[:, plane(i)] * s.slope2[:, plane(i)]).astype(BF)
        for bc in range(9):
            shift = (32 * (bc // 3 - 1) + 2 * (bc % 3 - 1)) % LANES
            s.wide_b[bc * C:(bc + 1) * C, plane(i)] = pltpu.roll(grad_pre, shift, 1) if shift else grad_pre
        if is_own:
            own_pre = (grad_pre.astype(F32) * own_lane).astype(BF)
            for a in range(3):
                s.lhs2[a * C:(a + 1) * C, plane(i + 2 * a - 2)] = own_pre

    def own_plane(i, carry):
        grad_plane(i + 2, True)
        return carry

    lax.fori_loop(0, 8, own_plane, 0, unroll=4)
    for i in (0, 1, 10, 11):
        grad_plane(i, False)

    pack_grads(s.grads_ref, 1, lax.dot_general(
        s.lhs2[...], s.wide2[:, 2 * LANES:14 * LANES], NT, preferred_element_type=F32), jnp.zeros((16, C), F32))
    s.out_b[...] = lax.dot_general(s.wb_ref[...], s.wide_b[...], TN, preferred_element_type=F32)

    def last_plane(q, carry):
        back = s.out_b[0:C, plane(q)] + s.out_b[C:2 * C, plane(q - 2)] + s.out_b[2 * C:3 * C, plane(q - 4)]
        _act, slope = elu_pair(s.pre1[q])
        grad_pre = (back * slope * own_lane).astype(BF)
        for a in range(3):
            s.lhs1[a * C:(a + 1) * C, plane(q + a - 4)] = grad_pre
        return carry

    lax.fori_loop(4, 12, last_plane, 0, unroll=4)

    pack_grads(s.grads_ref, 0, lax.dot_general(
        s.lhs1[...], s.wide1[:, 4 * LANES:14 * LANES], NT, preferred_element_type=F32), head_grad)


def finish_logits(s, logits_ref):
    logits_ref[12:16, :] = jnp.zeros((4, 128), F32)

    high = s.raw_logits[...].astype(BF)
    rest = s.raw_logits[...] - high.astype(F32)
    middle = rest.astype(BF)
    low = (rest - middle.astype(F32)).astype(BF)
    cell = lax.broadcasted_iota(jnp.int32, (1, 64), 1)
    source = ((cell >> 3) + 4) * 16 + (cell & 7) + 4
    pick = jnp.where(lax.broadcasted_iota(jnp.int32, (LANES, 64), 0) == source, 1.0, 0.0).astype(BF)
    parts = dot32(jnp.concatenate([high, middle, low], axis=0), pick)
    own_logits = (parts[0:64] + parts[64:128]) + parts[128:192]
    for x in range(8):
        for j in range(3):
            row = j * 4 + x // 2
            logits_ref[row:row + 1, x % 2 * 64:x % 2 * 64 + 64] = own_logits[x * 8 + j:x * 8 + j + 1]


def grad_sum_stage(s, g_ref, first_ref, second_ref, head_ref, meanwhile):
    pair_out, pair_in, send_buf, rs_buf, y_buf, done = (
        s.pair_out, s.pair_in, s.send_buf, s.rs_buf, s.y_buf, s.done)
    pair_send, pair_sem, rs_send, rs_sem = s.pair_send, s.pair_sem, s.rs_send, s.rs_sem
    y_send, y_sem, ag_send, ag_sem, last_send, last_sem = (
        s.y_send, s.y_sem, s.ag_send, s.ag_sem, s.last_send, s.last_sem)
    dp, sp = lax.axis_index("dp"), lax.axis_index("space")
    core, y = lax.rem(dp, 2), lax.div(dp, 2)
    n_y, n_sp = y_buf.shape[0], rs_buf.shape[0]
    partner = (dp + 1 - 2 * core, sp)

    def along(r):
        return lax.rem(sp + r, n_sp)

    def line(r):
        return (lax.rem(y + r, n_y) * 2 + core, sp)

    pair_out[...] = g_ref[1 - core].astype(BF)

    def remote(source, target, send, receive, device):
        return pltpu.make_async_remote_copy(
            src_ref=source, dst_ref=target, send_sem=send, recv_sem=receive, device_id=device, device_id_type=MESH)

    pair_copy = remote(pair_out, pair_in, pair_send, pair_sem, partner)
    pair_copy.start()
    pair_copy.wait_recv()
    send_buf[...] = (g_ref[core] + pair_in[...].astype(F32)).astype(BF)

    far_first = sorted(range(1, n_sp), key=lambda r: abs(n_sp // 2 - r))
    y_far_first = sorted(range(1, n_y), key=lambda r: abs(n_y // 2 - r))

    def rs_copy(r):
        return remote(send_buf.at[along(r)], rs_buf.at[r], rs_send.at[r], rs_sem.at[r], (dp, along(r)))

    def y_copy(r):
        return remote(y_buf.at[0], y_buf.at[r], y_send.at[r], y_sem.at[r], line(r))

    def ag_copy(r):
        return remote(done.at[core, sp], done.at[core, sp], ag_send.at[r], ag_sem.at[r], (dp, along(r)))

    def last_copy(r):
        slot = lax.rem(sp - r + n_sp, n_sp)
        return remote(done.at[core, slot], done.at[core, slot], last_send.at[r], last_sem.at[r], partner)

    for r in far_first:
        rs_copy(r).start()
    meanwhile()
    total = g_ref[core, sp] + pair_in[sp].astype(F32)
    for r in reversed(far_first):
        rs_copy(r).wait_recv()
        total = total + rs_buf[r].astype(F32)
    y_buf[0] = total.astype(BF)
    for r in y_far_first:
        y_copy(r).start()
    for r in range(1, n_y):
        y_copy(r).wait_recv()
    total = jnp.zeros(total.shape, F32)
    for d in range(n_y):
        total = total + y_buf[lax.rem(y - d + n_y, n_y)].astype(F32)
    done[core, sp] = total.astype(BF)
    for r in far_first:
        ag_copy(r).start()
    last_copy(0).start()
    for r in reversed(far_first):
        slot = lax.rem(sp - r + n_sp, n_sp)
        remote(done.at[core, slot], done.at[core, slot], ag_send.at[r], ag_sem.at[r], (dp, along(r))).wait_recv()
        last_copy(r).start()
    for r in range(n_sp):
        slot = lax.rem(sp - r + n_sp, n_sp)
        remote(done.at[1 - core, slot], done.at[1 - core, slot], last_send.at[r], last_sem.at[r], partner).wait_recv()

    for part, out in enumerate((first_ref, second_ref)):
        for group in range(9):
            a, rows = group // 3, slice(group % 3 * 16, group % 3 * 16 + 16)
            tail = done[part, 27 + group // 2]
            out[a * 9 + 8, rows, :] = tail[:, 64 * (group % 2):64 * (group % 2) + C]
            wide = jnp.concatenate([done[part, group * 3 + col] for col in range(3)], axis=1)
            for bc in range(8):
                out[a * 9 + bc, rows, :] = wide[:, bc * C:(bc + 1) * C]
    head_ref[12:15, 0:C] = done[0, 31].astype(F32)[0:3, 64:64 + C]

    pair_copy.wait_send()
    for r in range(1, n_sp):
        rs_copy(r).wait_send()
        ag_copy(r).wait_send()
    for r in range(1, n_y):
        y_copy(r).wait_send()
    for r in range(n_sp):
        last_copy(r).wait_send()


SCRATCH = dict(
    table=pltpu.SMEM((32,), jnp.int32),
    got=pltpu.VMEM((32, 4 * C + 16, 128), BF), own=pltpu.VMEM((4 * C + 16, 128), BF), wants=pltpu.VMEM((16, 128), F32),
    near=pltpu.VMEM((3, 18 * C, LANES), BF), near_t=pltpu.VMEM((3, 96, LANES), BF),
    faces=pltpu.VMEM((3, 18 * C, 3 * 128), BF), pick_ref=pltpu.VMEM((LANES, 3 * 128), BF),
    wide1=pltpu.VMEM((9 * C, 18 * LANES), BF), out1=pltpu.VMEM((3 * C, 18 * LANES), F32),
    pre1=pltpu.VMEM((16, C, LANES), F32),
    wide2=pltpu.VMEM((9 * C, 16 * LANES), BF), out2=pltpu.VMEM((3 * C, 16 * LANES), F32),
    wide_b=pltpu.VMEM((9 * C, 12 * LANES), BF), out_b=pltpu.VMEM((3 * C, 12 * LANES), F32),
    lhs2=pltpu.VMEM((3 * C, 12 * LANES), BF), lhs1=pltpu.VMEM((3 * C, 10 * LANES), BF),
    want=pltpu.VMEM((16, 12 * LANES), F32), mask_ref=pltpu.VMEM((3, 8, LANES), F32),
    mask2=pltpu.VMEM((8, 12 * LANES), F32), hid2=pltpu.VMEM((C, 12 * LANES), BF),
    slope2=pltpu.VMEM((C, 12 * LANES), F32), back2=pltpu.VMEM((C, 12 * LANES), F32),
    w1_ref=pltpu.VMEM((3 * C, 9 * C), BF), w2_ref=pltpu.VMEM((3 * C, 9 * C), BF),
    wb_ref=pltpu.VMEM((9 * C, 3 * C), BF), head_ref=pltpu.VMEM((16, C), F32),
    raw_logits=pltpu.VMEM((64, LANES), F32), grads_ref=pltpu.VMEM((2, 32, 16, 128), F32),
    pair_out=pltpu.VMEM((32, 16, 128), BF), pair_in=pltpu.VMEM((32, 16, 128), BF),
    send_buf=pltpu.VMEM((32, 16, 128), BF), rs_buf=pltpu.VMEM((32, 16, 128), BF),
    y_buf=pltpu.VMEM((N_Y, 16, 128), BF), done=pltpu.VMEM((2, 32, 16, 128), BF),
    send_sem=pltpu.SemaphoreType.DMA((64,)), recv_sem=pltpu.SemaphoreType.DMA((2, 32)),
    pair_send=pltpu.SemaphoreType.DMA, pair_sem=pltpu.SemaphoreType.DMA,
    rs_send=pltpu.SemaphoreType.DMA((32,)), rs_sem=pltpu.SemaphoreType.DMA((32,)),
    y_send=pltpu.SemaphoreType.DMA((N_Y,)), y_sem=pltpu.SemaphoreType.DMA((N_Y,)),
    ag_send=pltpu.SemaphoreType.DMA((32,)), ag_sem=pltpu.SemaphoreType.DMA((32,)),
    last_send=pltpu.SemaphoreType.DMA((32,)), last_sem=pltpu.SemaphoreType.DMA((32,)),
)


def whole_kernel(scale, ids_ref, features_ref, targets_ref, k1_ref, k2_ref, head_in_ref,
                 rows_ref, first_ref, second_ref, *scratch):
    s = SimpleNamespace(**dict(zip(SCRATCH, scratch)))
    sent = gather_stage(
        features_ref, targets_ref, s.got, s.own, s.wants, s.send_sem, s.recv_sem,
        lambda: prepare(s, ids_ref, k1_ref, k2_ref, head_in_ref))
    compute(s, scale)
    grad_sum_stage(s, s.grads_ref, first_ref, second_ref, rows_ref, lambda: finish_logits(s, rows_ref))
    for one in sent:
        one.wait_send()


def on_device(features, device_block, conv_first, conv_second, head_weight, targets):
    n_dp, n_sp = lax.axis_size("dp"), lax.axis_size("space")
    scale = (n_dp * n_sp * 3 * 512) ** (-0.5)
    vmem = pl.BlockSpec(memory_space=pltpu.VMEM)
    kernel = jax.ShapeDtypeStruct((27, C, C), BF)
    rows, first, second = pl.pallas_call(
        functools.partial(whole_kernel, scale),
        out_shape=(jax.ShapeDtypeStruct((16, 128), F32), kernel, kernel),
        in_specs=[pl.BlockSpec(memory_space=pltpu.SMEM)] + [vmem] * 5,
        out_specs=(vmem,) * 3,
        scratch_shapes=list(SCRATCH.values()),
        compiler_params=pltpu.CompilerParams(
            collective_id=0, has_side_effects=True, vmem_limit_bytes=60 * 1024 * 1024),
    )(device_block, features, targets.reshape(12, 128), conv_first.transpose(1, 0, 2), conv_second.transpose(1, 0, 2), head_weight)
    return (
        rows[:12].reshape(1, 1, 3, 512), first.transpose(1, 0, 2).astype(F32), second.transpose(1, 0, 2).astype(F32),
        rows[12:15, :C])


def solution(mesh):
    in_specs = (
        P("dp", "space", None, None),
        P("dp", None),
        P(),
        P(),
        P(),
        P("dp", "space", None, None),
    )
    out_specs = (P("dp", "space", None, None), P(), P(), P())
    return jax.shard_map(
        on_device, mesh=mesh, in_specs=in_specs, out_specs=out_specs, check_vma=False
    )
```
